32 devices in a mesh: lat: 8 (over z, y), ch: 4 (over x, core).
Axes of the slice: x: 2, y: 2, z: 4, core: 2. Of those that a mesh axis runs over, the one named last changes fastest.
Arguments:
- state: float32 [1, 24, 180, 768], P(None, 'lat', None, 'ch'), may hold values from -30 to 30
- norm_gains: bfloat16 [2, 768], P(None, 'ch'), may hold values from 0.099609375 to 1.8984375
- channel_biases: bfloat16 [3, 768], P(None, 'ch'), may hold values from -2 to 2
- filter_in: float32 [2, 8, 96, 96], P(None, 'ch'), may hold values from -0.4375 to 0.4375
- filter_in_bias: float32 [2, 8, 96], P(None, 'ch'), may hold values from -2 to 2
- filter_out: float32 [2, 8, 96, 96], P(None, 'ch'), may hold values from -0.4375 to 0.4375
- filter_out_bias: float32 [2, 8, 96], P(None, 'ch'), may hold values from -2 to 2
- up_weight: bfloat16 [768, 3072], P(None, 'ch'), may hold values from -0.21875 to 0.21875
- up_bias: bfloat16 [3072], P('ch'), may hold values from -2 to 2
- down_weight: bfloat16 [3072, 768], P('ch'), may hold values from -0.109375 to 0.109375
Outputs:
- final_state: float32 [1, 24, 180, 768], P(None, 'lat', None, 'ch')
The draws below stay inside these ranges and needn't reach their ends.
All inputs are finite; a program needn't handle non-finite values.
Results may differ from the reference program's by a relative error of at most 0.0012.
Values may be sent and summed in bfloat16 or wider, within the bound.
No kernel may reach another device: no remote copies, remote signals or barrier semaphores. Data moves between devices by JAX's collectives and lax.ppermute only.
A program may use at most 128 MiB of HBM per device.

```python
import math
import jax
import jax.numpy as jnp
from jax import lax

D = 768
FF = 3072
W = 180
NB = 8
M = 64
STEPS = 4
B = 1
H = 24
BS = 96


def draw_state(key, part):
    subkeys = jax.random.split(key, 3)
    channel_pos = jnp.arange(D).astype(jnp.float32) / D
    column_scale = 0.3 * jnp.exp(jax.random.uniform(subkeys[0], (D,), jnp.float32) * math.log(10.0)) * jnp.exp(channel_pos * 0.5 * math.log(3.0))
    channel_shift = 0.2 + 0.6 * channel_pos + 0.3 * jax.random.normal(subkeys[1], (D,), jnp.float32)
    value = jax.random.normal(subkeys[2], (B, H, W, D), jnp.float32) * column_scale + channel_shift
    return jnp.clip(value, -30.0, 30.0)


def block_scale(own_key, shape, cuts, smallest, high):
    level = 1.0
    for dim, shards_of in cuts:
        steps = jax.random.uniform(jax.random.fold_in(jax.random.fold_in(own_key, 6), dim), (shards_of,), jnp.float32, smallest / len(cuts), high / len(cuts))
        level = level * jnp.repeat(jnp.exp(steps), shape[dim] // shards_of).reshape((-1,) + (1,) * (len(shape) - 1 - dim))
    return level


def scatter_about(own_key, dims, scale, most, cuts=(), kind=jnp.bfloat16):
    values = scale * jax.random.normal(own_key, dims, jnp.float32)
    if cuts:
        values = values * block_scale(own_key, dims, cuts, -0.22, 0.18)
    return jnp.clip(values, -most, most).astype(kind)


def setup_inputs(seed: int = 0) -> dict:
    key_list = jax.random.split(jax.random.key(seed), 11)
    state = draw_state(jax.random.fold_in(key_list[10], 71), 0)
    norm_gains = jnp.clip(1.0 + 0.18 * jax.random.normal(key_list[1], (2, D), jnp.float32), 0.099609375, 1.8984375).astype(jnp.bfloat16)
    channel_biases = scatter_about(key_list[2], (3, D), 0.3, 2.0, ((1, 4),))
    filter_in = scatter_about(key_list[3], (2, NB, BS, BS), (2 * BS) ** -0.5, 0.4375, ((1, 4),), jnp.float32)
    filter_in_bias = scatter_about(key_list[4], (2, NB, BS), 0.3, 2.0, ((1, 4),), jnp.float32)
    filter_out = scatter_about(key_list[5], (2, NB, BS, BS), (2 * BS) ** -0.5, 0.4375, ((1, 4),), jnp.float32)
    filter_out_bias = scatter_about(key_list[6], (2, NB, BS), 0.3, 2.0, ((1, 4),), jnp.float32)
    up_weight = scatter_about(key_list[7], (D, FF), D ** -0.5, 0.21875, ((1, 4),))
    up_bias = scatter_about(key_list[8], (FF,), 0.3, 2.0, ((0, 4),))
    down_weight = scatter_about(key_list[9], (FF, D), FF ** -0.5, 0.109375, ((0, 4),))
    return dict(state=state, norm_gains=norm_gains, channel_biases=channel_biases, filter_in=filter_in, filter_in_bias=filter_in_bias, filter_out=filter_out, filter_out_bias=filter_out_bias, up_weight=up_weight, up_bias=up_bias, down_weight=down_weight)


EPS = 1e-05
SHRINK = 0.01
HIGH = lax.Precision.HIGHEST

def longitude_tables(width, modes):
    column = jnp.arange(width, dtype=jnp.int32)[:, None]
    order = jnp.arange(modes, dtype=jnp.int32)[None, :]
    angle = 2.0 * math.pi / width * (column * order % width).astype(jnp.float32)
    doubled = jnp.where(order == 0, 1.0, 2.0).astype(jnp.float32)
    return (jnp.cos(angle), jnp.sin(angle), jnp.cos(angle) * doubled, jnp.sin(angle) * doubled)

def latitude_tables(height):
    column = jnp.arange(height, dtype=jnp.int32)[:, None]
    order = jnp.arange(height, dtype=jnp.int32)[None, :]
    angle = 2.0 * math.pi / height * (column * order % height).astype(jnp.float32)
    return (jnp.cos(angle), jnp.sin(angle))

def layer_norm(values, gain, shift):
    mean = lax.optimization_barrier(jnp.sum(values, -1, keepdims=True)) / values.shape[-1]
    spread = lax.optimization_barrier(jnp.sum(values * values, -1, keepdims=True)) / values.shape[-1] - mean * mean
    return (values - mean) * lax.rsqrt(spread + EPS) * gain + shift

def soft_shrink(values):
    return jnp.where(values > SHRINK, values - SHRINK, jnp.where(values < -SHRINK, values + SHRINK, 0.0))

def block_apply(left, matrix):
    return jnp.einsum('bkmnj,nji->bkmni', left, matrix, precision=HIGH)

def spectral_mlp(real_part, imag_part, filter_in, filter_in_bias, filter_out, filter_out_bias):
    shape = real_part.shape
    blocks = filter_in.shape[1]
    size = filter_in.shape[2]
    real_blocks = real_part.reshape(shape[:-1] + (blocks, size))
    imag_blocks = imag_part.reshape(shape[:-1] + (blocks, size))
    first_real = jax.nn.relu(block_apply(real_blocks, filter_in[0]) - block_apply(imag_blocks, filter_in[1]) + filter_in_bias[0])
    first_imag = jax.nn.relu(block_apply(imag_blocks, filter_in[0]) + block_apply(real_blocks, filter_in[1]) + filter_in_bias[1])
    second_real = block_apply(first_real, filter_out[0]) - block_apply(first_imag, filter_out[1]) + filter_out_bias[0]
    second_imag = block_apply(first_imag, filter_out[0]) + block_apply(first_real, filter_out[1]) + filter_out_bias[1]
    return (soft_shrink(second_real).reshape(shape), soft_shrink(second_imag).reshape(shape))

def spectral_filter(normed, filter_in, filter_in_bias, filter_out, filter_out_bias):
    height = normed.shape[1]
    width = normed.shape[2]
    lon_cos, lon_sin, back_cos, back_sin = longitude_tables(width, M)
    lat_cos, lat_sin = latitude_tables(height)
    scale = 1.0 / math.sqrt(height * width)
    real_lon = jnp.einsum('bhwd,wm->bhmd', normed, lon_cos, precision=HIGH)
    imag_lon = -jnp.einsum('bhwd,wm->bhmd', normed, lon_sin, precision=HIGH)
    real_spec = (jnp.einsum('kh,bhmd->bkmd', lat_cos, real_lon, precision=HIGH) + jnp.einsum('kh,bhmd->bkmd', lat_sin, imag_lon, precision=HIGH)) * scale
    imag_spec = (jnp.einsum('kh,bhmd->bkmd', lat_cos, imag_lon, precision=HIGH) - jnp.einsum('kh,bhmd->bkmd', lat_sin, real_lon, precision=HIGH)) * scale
    out_real, out_imag = spectral_mlp(real_spec, imag_spec, filter_in, filter_in_bias, filter_out, filter_out_bias)
    real_rows = jnp.einsum('kh,bkmd->bhmd', lat_cos, out_real, precision=HIGH) - jnp.einsum('kh,bkmd->bhmd', lat_sin, out_imag, precision=HIGH)
    imag_rows = jnp.einsum('kh,bkmd->bhmd', lat_cos, out_imag, precision=HIGH) + jnp.einsum('kh,bkmd->bhmd', lat_sin, out_real, precision=HIGH)
    back = jnp.einsum('bhmd,wm->bhwd', real_rows, back_cos, precision=HIGH) - jnp.einsum('bhmd,wm->bhwd', imag_rows, back_sin, precision=HIGH)
    return back * scale

def reference(state, norm_gains, channel_biases, filter_in, filter_in_bias, filter_out, filter_out_bias, up_weight, up_bias, down_weight):
    gains = norm_gains.astype(jnp.float32)
    shifts = channel_biases.astype(jnp.float32)
    values = state
    for step_index in range(STEPS):
        normed = layer_norm(values, gains[0], shifts[0])
        values = values + spectral_filter(normed, filter_in, filter_in_bias, filter_out, filter_out_bias) + normed
        normed_two = layer_norm(values, gains[1], shifts[1]).astype(jnp.bfloat16)
        flat = normed_two.reshape(-1, normed_two.shape[-1])
        pre = jnp.dot(flat, up_weight, preferred_element_type=jnp.float32) + up_bias.astype(jnp.float32)
        hidden = jax.nn.gelu(pre, approximate=False).astype(jnp.bfloat16)
        mixed = jnp.dot(hidden, down_weight, preferred_element_type=jnp.float32) + shifts[2]
        values = values + mixed.reshape(values.shape)
    return values
```

```python
import math

import jax
import jax.numpy as jnp
import numpy as np
from jax import lax
from jax.experimental import pallas as pl
from jax.experimental.pallas import tpu as pltpu
from jax.sharding import PartitionSpec as P


D = 768
M = 64
STEPS = 4
EPS = 1e-05
SHRINK = 0.01
HALF = 64
LANES = 128
BF = jnp.bfloat16
F32 = jnp.float32


class Plan:
    def __init__(self, lat, ch, rows, width):
        self.lat, self.ch, self.rows, self.width = lat, ch, rows, width
        self.height = rows * lat
        self.short = width // ch
        self.padded = -(-self.short // 16) * 16
        self.tokens = rows * self.padded
        self.classes = self.short // 2 + 1
        self.per = -(-self.classes // lat)
        self.wide = D // ch
        self.units = self.wide // HALF
        self.items = rows * self.per
        spare = self.items % 8
        if self.items > 8 and spare and spare * self.units <= 8:
            self.main, self.left = self.items - spare, spare
        else:
            self.main, self.left = -(-self.items // 8) * 8, 0
        self.message = self.units * self.main + (8 if self.left else 0)
        slots = 0
        while (slots // 2) * self.short + (slots % 2) * (self.short - self.short // 2) < M:
            slots += 1
        self.slots = slots
        self.modes = self.per * slots * self.height
        self.peers = lat * ch
        self.spare = self.padded - self.short
        self.packed = self.tokens + self.tokens // 2
        hj = np.arange(self.main)
        self.item_h = np.where(hj < self.items, hj // self.per, 0)
        self.item_j = np.where(hj < self.items, hj % self.per, -1)
        tail = self.main + np.arange(self.left)
        self.tail_h, self.tail_j = tail // self.per, tail % self.per


def split_np(table):
    hi = table.astype(np.float32).astype(BF)
    lo = (table - hi.astype(np.float64)).astype(np.float32).astype(BF)
    return hi, lo


def short_tables(plan):
    g = np.arange(plan.lat)
    item_g = np.concatenate([np.repeat(g, plan.main), np.repeat(g, plan.left)])
    item_h = np.concatenate([np.tile(plan.item_h, plan.lat), np.tile(plan.tail_h, plan.lat)])
    item_j = np.concatenate([np.tile(plan.item_j, plan.lat), np.tile(plan.tail_j, plan.lat)])
    order = item_g * plan.per + item_j
    good = (item_j >= 0) & (order < plan.classes)
    tok_h = np.repeat(np.arange(plan.rows), plan.padded)
    tok_a = np.tile(np.arange(plan.padded), plan.rows)
    mask = good[:, None] & (item_h[:, None] == tok_h[None]) & (tok_a[None] < plan.short)
    angle = 2 * np.pi / plan.short * (order[:, None] * tok_a[None] % plan.short)
    cos, sin = np.cos(angle) * mask, np.sin(angle) * mask
    forward = np.concatenate([cos, -sin], 0)
    inverse = np.concatenate([cos.T, -sin.T], 1)
    return np.stack(split_np(forward)), np.stack(split_np(inverse))


def mode_places(plan):
    j, t, k = (
        v.reshape(-1)
        for v in np.meshgrid(
            np.arange(plan.per), np.arange(plan.slots), np.arange(plan.height), indexing="ij"
        )
    )
    peer = np.arange(plan.peers)
    col_p = np.concatenate([np.repeat(peer, plan.main), np.repeat(peer, plan.left)])
    col_h = np.concatenate([np.tile(plan.item_h, plan.peers), np.tile(plan.tail_h, plan.peers)])
    col_j = np.concatenate([np.tile(plan.item_j, plan.peers), np.tile(plan.tail_j, plan.peers)])
    col_h = (col_p // plan.ch) * plan.rows + col_h
    none = np.zeros_like(j)
    row = np.stack([j, t % 2, (t + 1) // 2, k] + [none] * 4).astype(np.float32)
    none = np.zeros_like(col_p)
    col = np.stack([col_p % plan.ch, col_h, col_j] + [none] * 5).astype(np.float32)
    return row, col


def cos_sin(turns):
    turns = turns - jnp.floor(turns + 0.5)
    quarter = jnp.floor(turns * 4.0 + 0.5)
    x = (turns - quarter * 0.25) * (2.0 * math.pi)
    y = x * x
    sin = x * (1 + y * (-1 / 6 + y * (1 / 120 + y * (-1 / 5040 + y * (1 / 362880)))))
    cos = 1 + y * (-0.5 + y * (1 / 24 + y * (-1 / 720 + y * (1 / 40320 - y * (1 / 3628800)))))
    odd = jnp.abs(quarter) == 1.0
    c, s = jnp.where(odd, sin, cos), jnp.where(odd, cos, sin)
    c = jnp.where((quarter == 1.0) | (jnp.abs(quarter) == 2.0), -c, c)
    s = jnp.where((quarter == -1.0) | (jnp.abs(quarter) == 2.0), -s, s)
    return c, s


def mode_table(plan, first_class, row, col):
    j, odd, times, k = row
    q, h, col_j = col
    order = first_class + j
    mode = times * plan.short + jnp.where(odd == 1.0, -order, order)
    fine = (mode < M) & (order < plan.classes)
    fine = fine & ((order > 0.0) | (times == 0.0) | (odd == 1.0))
    fine = fine & ((2.0 * order != plan.short) | (odd == 0.0))
    scale = 1.0 / math.sqrt(plan.height * plan.width)
    weight = jnp.where(fine, scale, 0.0)
    doubled = jnp.where(mode == 0.0, 1.0, 2.0)
    turn = jnp.where(odd == 1.0, 1.0, -1.0)
    product = k * h
    product = product - plan.height * jnp.floor(product * (1.0 / plan.height) + 1e-4)
    cos, sin = cos_sin(mode * q * (1.0 / plan.width) + product * (1.0 / plan.height))
    keep = jnp.where(j == col_j, weight, 0.0)
    return cos * keep, sin * (keep * turn), doubled


def split(value):
    hi = value.astype(BF)
    return hi, (value - hi.astype(F32)).astype(BF)


def dot(a, b):
    return jnp.dot(a, b, preferred_element_type=F32)


def low_lanes(shape):
    return lax.broadcasted_iota(jnp.int32, shape, len(shape) - 1) % LANES < HALF


def swap(value):
    return pltpu.roll(value, HALF, 1)


def norm(values, gain, shift):
    mean = jnp.sum(values, -1, keepdims=True) * (1.0 / D)
    spread = jnp.sum(values * values, -1, keepdims=True) * (1.0 / D) - mean * mean
    return (values - mean) * lax.rsqrt(spread + EPS) * gain + shift


def emit_wire(plan, normed, fhi, flo, wire_ref, scratch):
    hi, lo = split(normed)
    spec = dot(fhi[...], hi) + dot(flo[...], hi) + dot(fhi[...], lo)
    count = plan.lat * plan.main
    extra = plan.lat * plan.left
    half = count + extra
    low = low_lanes((half, LANES))
    for tile in range(D // LANES):
        lanes = slice(tile * LANES, (tile + 1) * LANES)
        re, im = spec[:half, lanes], spec[half:, lanes]
        pair = (jnp.where(low, re, swap(im)), jnp.where(low, swap(re), im))
        for which in range(2):
            c, u = divmod(2 * tile + which, plan.units)
            part = pair[which]
            scratch[:, c, u * plan.main : (u + 1) * plan.main, :] = part[:count].reshape(
                plan.lat, plan.main, LANES
            )
            for spot in range(plan.left):
                row = plan.units * plan.main + u * plan.left + spot
                for g in range(plan.lat):
                    at = count + g * plan.left + spot
                    scratch[g, c, row : row + 1, :] = part[at : at + 1]
    if plan.left:
        first = plan.units * (plan.main + plan.left)
        if first < plan.message:
            scratch[:, :, first:, :] = jnp.zeros(
                (plan.lat, plan.ch, plan.message - first, LANES), F32
            )
    wire_ref[...] = scratch[...].reshape(plan.peers, plan.message, LANES).astype(BF)


def read_wire(plan, wire_ref, ghi, glo, scratch):
    scratch[...] = wire_ref[...].astype(F32).reshape(plan.lat, plan.ch, plan.message, LANES)
    count = plan.lat * plan.main
    half = count + plan.lat * plan.left
    low = low_lanes((half, LANES))

    def unit(index):
        c, u = divmod(index, plan.units)
        parts = [scratch[:, c, u * plan.main : (u + 1) * plan.main, :].reshape(count, LANES)]
        for g in range(plan.lat):
            for spot in range(plan.left):
                row = plan.units * plan.main + u * plan.left + spot
                parts.append(scratch[g, c, row : row + 1, :])
        return jnp.concatenate(parts, 0) if len(parts) > 1 else parts[0]

    tiles = []
    for tile in range(D // LANES):
        a, b = unit(2 * tile), unit(2 * tile + 1)
        re = jnp.where(low, a, swap(b))
        im = jnp.where(low, swap(a), b)
        tiles.append(jnp.concatenate([re, im], 0).astype(BF))
    right = jnp.concatenate(tiles, 1)
    return dot(ghi[...], right) + dot(glo[...], right)


def pack(values):
    half = values.shape[0] // 2
    tail = values[:, LANES:]
    return jnp.concatenate([values[:, :LANES], jnp.concatenate([tail[:half], tail[half:]], 1)], 0)


def unpack(message):
    tokens = message.shape[0] // 3 * 2
    tail = message[tokens:]
    tail = jnp.concatenate([tail[:, :HALF], tail[:, HALF:]], 0)
    return jnp.concatenate([message[:tokens], tail], 1)


def pack_kernel(plan, state_ref, gain_hbm, bias_hbm, up_hbm, out_ref, scratch, body, tail, *refs):
    gain_ref, bias_ref, up_ref, sem = refs
    copies = fetch([gain_hbm, bias_hbm, up_hbm], [gain_ref, bias_ref, up_ref], sem)
    body[...] = state_ref[:, :, :LANES]
    tail[:, :, :HALF] = state_ref[:, :, LANES:]
    for copy in copies:
        copy.wait()
    line = up_ref[...].astype(F32)
    small = [gain_ref[...].astype(F32), bias_ref[...].astype(F32)]
    small += [line[:, n * plan.wide : (n + 1) * plan.wide] for n in range(plan.ch)]
    small = jnp.concatenate(small, 0)
    count = small.shape[0]
    scratch[...] = jnp.zeros(scratch.shape, F32)
    for n in range(count):
        h, s = divmod(n, plan.spare)
        at = h * plan.padded + plan.short + s
        scratch[at : at + 1, :] = small[n : n + 1]
    for q in range(plan.ch):
        for h in range(plan.rows):
            at = h * plan.padded
            every = pl.ds(q, plan.short, stride=plan.ch)
            scratch[at : at + plan.short, :LANES] = body[h, every, :]
            scratch[at : at + plan.short, LANES:] = tail[h, every, :][:, :HALF]
        out_ref[q] = pack(scratch[...])


def unpack_kernel(plan, got_ref, out_ref, body, tail):
    for q in range(plan.ch):
        values = unpack(got_ref[q])
        wide = jnp.concatenate([values[:, LANES:], values[:, LANES:]], 1)
        for h in range(plan.rows):
            at = slice(h * plan.padded, h * plan.padded + plan.short)
            every = pl.ds(q, plan.short, stride=plan.ch)
            body[h, every, :] = values[at, :LANES]
            tail[h, every, :] = wide[at]
    out_ref[:, :, :LANES] = body[...]
    out_ref[:, :, LANES:] = tail[:, :, :HALF]


def fetch(sources, targets, sem):
    copies = [pltpu.make_async_copy(a, b, sem.at[n]) for n, (a, b) in enumerate(zip(sources, targets))]
    for copy in copies:
        copy.start()
    return copies


def parts_kernel(me_ref, up_ref, down_ref, up_out, near_out, rest_out, *refs):
    mids, sem = refs[:3], refs[3]
    half, third = up_out.shape[1], near_out.shape[0]
    at = pl.multiple_of(me_ref[2] * half, LANES)
    to = pl.multiple_of(me_ref[2] * third, LANES)
    into = fetch(
        [up_ref.at[:, pl.ds(at, half)], down_ref.at[pl.ds(to, third), :], down_ref.at[2 * third :, :]],
        mids,
        sem,
    )
    away = []
    for n, out in enumerate((up_out, near_out, rest_out)):
        into[n].wait()
        away.append(pltpu.make_async_copy(mids[n], out, sem.at[3 + n]))
        away[n].start()
    for copy in away:
        copy.wait()


def prep_kernel(plan, me_ref, rowv, colv, rowt, colt, fin, finb, fout, foutb, *refs):
    count = len(refs) // 2
    outs, (chi, clo, ehi, elo, w1h, w1l, w2h, w2l, b1, b2) = refs[:count], refs[count:-1]
    sem = refs[-1]
    copies = [pltpu.make_async_copy(a, b, sem.at[n]) for n, (a, b) in enumerate(zip(refs[count:], outs))]
    first = (me_ref[0] * plan.per).astype(F32)
    size = plan.modes
    wide = plan.peers * (plan.main + plan.left)
    rows = [rowv[:, n : n + 1] for n in range(4)]
    cols = [colv[n : n + 1, :] for n in range(3)]
    cos, sin, _ = mode_table(plan, first, rows, cols)
    chi[:, :wide], clo[:, :wide] = split(cos)
    chi[:, wide:], clo[:, wide:] = split(sin)
    copies[0].start()
    copies[1].start()
    rows = [rowt[n : n + 1, :] for n in range(4)]
    cols = [colt[:, n : n + 1] for n in range(3)]
    cos, sin, doubled = mode_table(plan, first, rows, cols)
    ehi[:, :size], elo[:, :size] = split(cos * doubled)
    ehi[:, size:], elo[:, size:] = split(-sin * doubled)
    copies[2].start()
    copies[3].start()
    for weights, bias, high, low, out in ((fin, finb, w1h, w1l, b1), (fout, foutb, w2h, w2l, b2)):
        blocks, channels = weights.shape[1], weights.shape[2]
        full = []
        for p in range(2):
            lines = []
            for n in range(blocks):
                cells = [jnp.zeros((channels, channels), F32)] * blocks
                cells[n] = weights[p, n]
                lines.append(jnp.concatenate(cells, 1))
            full.append(jnp.concatenate(lines, 0))
        for u in range(plan.units):
            at = slice(u * HALF, (u + 1) * HALF)
            real, imag = full[0][at], full[1][at]
            for p, (left, right) in enumerate(((real, imag), (-imag, real))):
                cells = []
                for v in range(plan.units):
                    cells += [left[:, v * HALF : (v + 1) * HALF], right[:, v * HALF : (v + 1) * HALF]]
                row = jnp.concatenate(cells, 1)
                to = slice((2 * u + p) * HALF, (2 * u + p + 1) * HALF)
                high[to, :], low[to, :] = split(row)
        lines = [jnp.concatenate([bias[p, n : n + 1] for n in range(blocks)], 1) for p in range(2)]
        cells = []
        for v in range(plan.units):
            cells += [line[:, v * HALF : (v + 1) * HALF] for line in lines]
        out[...] = jnp.concatenate(cells, 1)
    for copy in copies[4:]:
        copy.start()
    for copy in copies:
        copy.wait()


def start_kernel(plan, me_ref, got_ref, tab_hbm, sum_hbm, wire_ref, par_hbm, *refs):
    scratch, tab, sum_ref, par_ref, sem = refs
    bias_ref = par_ref.at[8:16]
    copies = fetch([tab_hbm], [tab], sem)
    got = [unpack(got_ref[c]) for c in range(plan.ch)]
    full = jnp.concatenate(got, 1)
    rows = []
    for h in range(plan.rows):
        for s in range(plan.spare):
            rows.append(h * plan.padded + plan.short + s)
    for n in range(5):
        par_ref[n : n + 1, :] = full[rows[n] : rows[n] + 1, :]
    par_ref[5:8, :] = jnp.zeros((3, D), F32)
    bias_ref[...] = jnp.zeros(bias_ref.shape, F32)
    for s in range(plan.ch):
        source = unpack(got_ref[me_ref[1] ^ s])
        parts = [source[rows[5 + n] : rows[5 + n] + 1, :] for n in range(plan.ch)]
        line = jnp.concatenate(parts, 1)
        bias_ref[s : s + 1, :] = line
    inside = lax.broadcasted_iota(jnp.int32, (plan.tokens, 1), 0) % plan.padded < plan.short
    values = jnp.where(inside, full, 0.0)
    normed = norm(values, par_ref[0:1, :], par_ref[2:3, :])
    sum_ref[...] = values + normed
    copies.append(pltpu.make_async_copy(sum_ref, sum_hbm, sem.at[1]))
    copies.append(pltpu.make_async_copy(par_ref, par_hbm, sem.at[2]))
    copies[1].start()
    copies[2].start()
    copies[0].wait()
    emit_wire(plan, normed, tab.at[0], tab.at[1], wire_ref, scratch)
    copies[1].wait()
    copies[2].wait()


def token_kernel(plan, first, last, *refs):
    copies = []
    if first:
        me_ref, wire_in = refs[:2]
        sources, refs = refs[2:20], refs[20:]
        (sum_out, wire_out, up_all, down_all), refs = refs[:4], refs[4:]
        scratch, sem, (sum_in, ahead, behind, par_ref) = refs[0], refs[1], refs[2:]
        shard = up_all.shape[1] // plan.ch
        half, third = shard // 2, shard // 3
        y = me_ref[2]
        copies = fetch(sources[:4], (sum_in, ahead, behind, par_ref), sem)
        groups = []
        weights = sources[4:]
        for s in range(plan.ch):
            at = s * shard
            if s < plan.ch // 2:
                ups, downs = weights[:1], weights[1:2]
                weights = weights[2:]
                ups = [(ups[0], up_all.at[:, at : at + shard])]
                downs = [(downs[0], down_all.at[at : at + shard, :])]
            else:
                ups, downs = weights[:2], weights[2:5]
                spots = [pl.multiple_of(at + n * half, LANES) for n in (y, 1 - y)]
                ups = [(w, up_all.at[:, pl.ds(n, half)]) for w, n in zip(ups, spots)]
                spots = [pl.multiple_of(at + n * third, LANES) for n in (y, 1 - y)]
                spots.append(at + 2 * third)
                downs = [(w, down_all.at[pl.ds(n, third), :]) for w, n in zip(downs, spots)]
                weights = weights[5:]
            group = []
            for source, target in ups + downs:
                count = len(copies)
                copies.append(pltpu.make_async_copy(source, target, sem.at[count]))
                copies[-1].start()
                group.append(copies[-1])
            groups.append(group)
        for copy in copies[:4]:
            copy.wait()
    else:
        wire_in, sum_in, ahead, behind, par_ref, up_all, down_all = refs[:7]
        outs, scratch = refs[7:-1], refs[-1]
        shard = up_all.shape[1] // plan.ch
        half = shard // 2
    values = sum_in[...] + read_wire(plan, wire_in, behind.at[0], behind.at[1], scratch)
    normed = norm(values, par_ref[1:2, :], par_ref[3:4, :]).astype(BF)
    mixed = par_ref[4:5, :]
    for s in range(2 * plan.ch):
        if first and s % 2 == 0:
            for copy in groups[s // 2]:
                copy.wait()
        at = slice((s % 2) * half, (s % 2 + 1) * half)
        cut = slice(s * half, (s + 1) * half)
        bias = par_ref[8 + s // 2 : 9 + s // 2, at]
        pre = dot(normed, up_all[:, cut]) + bias
        hidden = (0.5 * pre * (1.0 + lax.erf(pre * math.sqrt(0.5)))).astype(BF)
        mixed = mixed + dot(hidden, down_all[cut, :])
    values = values + mixed
    if last:
        for c in range(plan.ch):
            outs[0][c] = pack(values[:, c * plan.wide : (c + 1) * plan.wide])
        return
    if not first:
        sum_out, wire_out = outs
    normed = norm(values, par_ref[0:1, :], par_ref[2:3, :])
    sum_out[...] = values + normed
    emit_wire(plan, normed, ahead.at[0], ahead.at[1], wire_out, scratch)


def spectral_kernel(plan, far, wire_in, *refs):
    copies = []
    if far:
        sources, refs = refs[:11], refs[11:]
        wire_out, scratch, sem, mids = refs[0], refs[1], refs[2], refs[3:]
        copies = fetch(sources, mids, sem)
    else:
        mids, (wire_out, scratch) = refs[:11], refs[11:]
    chi, clo, ehi, elo, w1h, w1l, w2h, w2l, b1, b2, sign_ref = mids
    scratch[...] = wire_in[...].astype(F32)
    count = plan.peers * plan.main
    half = count + plan.peers * plan.left
    low = low_lanes((half, LANES))
    pieces = []
    for u in range(plan.units):
        parts = [scratch[:, u * plan.main : (u + 1) * plan.main, :].reshape(count, LANES)]
        for p in range(plan.peers if plan.left else 0):
            row = plan.units * plan.main + u * plan.left
            parts.append(scratch[p, row : row + plan.left, :])
        data = jnp.concatenate(parts, 0) if len(parts) > 1 else parts[0]
        turned = swap(data)
        turned = jnp.where(low, -turned, turned)
        pieces.append(jnp.concatenate([data, turned], 0).astype(BF))
    right = jnp.concatenate(pieces, 1)

    def ready(*which):
        for n in which if far else ():
            copies[n].wait()

    ready(0, 1, 10)
    spec = dot(chi[...], right) + dot(clo[...], right)
    sign = jnp.concatenate([sign_ref[...]] * plan.units, 1)
    spec = spec * sign

    def layer(value, wh, wl, bias):
        hi, lo = split(value)
        return dot(hi, wh[...]) + dot(hi, wl[...]) + dot(lo, wh[...]) + bias[...]

    ready(4, 5, 8)
    first = jnp.maximum(layer(spec, w1h, w1l, b1), 0.0)
    ready(6, 7, 9)
    second = layer(first, w2h, w2l, b2)
    shrunk = jnp.where(
        second > SHRINK, second - SHRINK, jnp.where(second < -SHRINK, second + SHRINK, 0.0)
    )
    shrunk = shrunk * sign
    low = low_lanes((plan.modes, LANES))
    pieces = []
    for u in range(plan.units):
        part = shrunk[:, u * LANES : (u + 1) * LANES]
        turned = swap(part)
        pieces.append(jnp.concatenate([part, jnp.where(low, -turned, turned)], 0))
    hi, lo = split(jnp.concatenate(pieces, 1))
    ready(2, 3)
    back = dot(ehi[...], hi) + dot(elo[...], hi) + dot(ehi[...], lo)
    for u in range(plan.units):
        part = back[:, u * LANES : (u + 1) * LANES]
        scratch[:, u * plan.main : (u + 1) * plan.main, :] = part[:count].reshape(
            plan.peers, plan.main, LANES
        )
        row = plan.units * plan.main + u * plan.left
        for p in range(plan.peers if plan.left else 0):
            at = count + p * plan.left
            scratch[p, row : row + plan.left, :] = part[at : at + plan.left]
    wire_out[...] = scratch[...].astype(BF)


def call(body, outs, operands, scratch, flops, smem=0, far_in=0, far_out=(), grant=20):
    vmem = pl.BlockSpec(memory_space=pltpu.VMEM)
    anywhere = pl.BlockSpec(memory_space=pl.ANY)
    flat, tree = jax.tree.flatten(outs)
    out_specs = [anywhere if n in far_out else vmem for n in range(len(flat))]
    return pl.pallas_call(
        body,
        out_shape=outs,
        in_specs=[pl.BlockSpec(memory_space=pltpu.SMEM)] * smem
        + [vmem] * (len(operands) - smem - far_in)
        + [anywhere] * far_in,
        out_specs=jax.tree.unflatten(tree, out_specs),
        scratch_shapes=scratch,
        compiler_params=pltpu.CompilerParams(vmem_limit_bytes=grant * 2**20),
        cost_estimate=pl.CostEstimate(flops=flops, bytes_accessed=2**20, transcendentals=0),
    )(*operands)


def local(
    state,
    norm_gains,
    channel_biases,
    filter_in,
    filter_in_bias,
    filter_out,
    filter_out_bias,
    up_weight,
    up_bias,
    down_weight,
):
    _, rows, width, wide = state.shape
    plan = Plan(lax.axis_size("lat"), lax.axis_size("ch"), rows, width)
    ch = plan.ch
    far = ch // 2
    both = ("lat", "ch")
    assert plan.spare * rows >= 5 + ch and up_bias.shape[0] == ch * wide
    lat_me = lax.axis_index("lat").astype(jnp.int32)
    me = jnp.stack([lat_me, lax.axis_index("ch").astype(jnp.int32), lat_me % 2])

    def across(value, step):
        return lax.ppermute(value, "ch", [(i, i ^ step) for i in range(ch)])

    def beside(value):
        return lax.ppermute(value, "lat", [(i, i ^ 1) for i in range(plan.lat)])

    def exchange(value, axes):
        return lax.all_to_all(value, axes, 0, 0, tiled=True)

    def after(value, token):
        return lax.optimization_barrier((value, token))[0]

    message = jax.ShapeDtypeStruct((ch, plan.packed, LANES), F32)
    tokens = call(
        lambda *r: pack_kernel(plan, *r),
        message,
        (state[0], norm_gains, channel_biases, up_bias.reshape(1, ch * wide)),
        [pltpu.VMEM((plan.tokens, wide), F32)]
        + [pltpu.VMEM((rows, width, LANES), F32)] * 2
        + [pltpu.VMEM(v.shape, BF) for v in (norm_gains, channel_biases, up_bias.reshape(1, -1))]
        + [pltpu.SemaphoreType.DMA((3,))],
        10**8,
        far_in=3,
        grant=58,
    )
    got = exchange(tokens, "ch")

    half, third = up_weight.shape[1] // 2, down_weight.shape[0] // 3
    parts = [
        jax.ShapeDtypeStruct((up_weight.shape[0], half), BF),
        jax.ShapeDtypeStruct((third, down_weight.shape[1]), BF),
        jax.ShapeDtypeStruct((third, down_weight.shape[1]), BF),
    ]
    up_part, near_part, rest_part = call(
        parts_kernel,
        tuple(parts),
        (me, up_weight, down_weight),
        [pltpu.VMEM(t.shape, BF) for t in parts] + [pltpu.SemaphoreType.DMA((6,))],
        10**6,
        smem=1,
        far_in=2,
        far_out=(0, 1, 2),
        grant=58,
    )
    up_a = across(up_part, far)
    up_c, down_c = across(up_weight, 1), across(down_weight, 1)

    ahead, behind = (jnp.asarray(table) for table in short_tables(plan))
    odd = np.tile(np.repeat(np.arange(plan.slots) % 2, plan.height), plan.per)
    sign = np.where((odd[:, None] == 1) & (np.arange(LANES)[None] >= HALF), -1.0, 1.0)
    sign = sign.astype(np.float32)

    wire = jax.ShapeDtypeStruct((plan.peers, plan.message, LANES), BF)
    held = jax.ShapeDtypeStruct((plan.tokens, D), F32)
    scratch = [pltpu.VMEM((plan.lat, ch, plan.message, LANES), F32)]
    params = jax.ShapeDtypeStruct((16, D), F32)
    total, sent, params = call(
        lambda *r: start_kernel(plan, *r),
        (held, wire, params),
        (me, got, ahead),
        scratch
        + [pltpu.VMEM(t.shape, t.dtype) for t in (ahead, held, params)]
        + [pltpu.SemaphoreType.DMA((3,))],
        10**9,
        smem=1,
        far_in=1,
        far_out=(0, 2),
        grant=58,
    )
    row, col = mode_places(plan)
    lines = plan.peers * (plan.main + plan.left)
    tables = [
        jax.ShapeDtypeStruct(dims, BF)
        for dims in [(plan.modes, 2 * lines)] * 2
        + [(lines, 2 * plan.modes)] * 2
        + [(2 * wide, 2 * wide)] * 4
    ] + [jax.ShapeDtypeStruct((1, 2 * wide), F32)] * 2
    spectral_in = call(
        lambda *r: prep_kernel(plan, *r),
        tuple(tables),
        (after(me, sent), row.T, col, row, col.T, filter_in, filter_in_bias, filter_out, filter_out_bias),
        [pltpu.VMEM(t.shape, t.dtype) for t in tables] + [pltpu.SemaphoreType.DMA((len(tables),))],
        10**8,
        smem=1,
        far_out=range(len(tables)),
        grant=58,
    )
    for step_index in range(STEPS):
        first, last = step_index == 0, step_index == STEPS - 1
        arrived = exchange(sent, both)
        if first:
            down_a = across(near_part, far)
            up_b = beside(up_a)
            up_ac = across(up_a, 1)
        tabs = (*spectral_in, sign)
        mids = [pltpu.VMEM(t.shape, t.dtype) for t in tabs] if first else []
        sent = call(
            lambda *r: spectral_kernel(plan, first, *r),
            wire,
            (arrived, *tabs),
            [pltpu.VMEM((plan.peers, plan.message, LANES), F32)]
            + ([pltpu.SemaphoreType.DMA((len(tabs),))] if first else [])
            + mids,
            10**9,
            far_in=len(mids),
            grant=58 if first else 20,
        )
        if first:
            down_b = beside(after(down_a, sent))
            down_ac = across(after(down_a, sent), 1)
            up_bc = across(after(up_b, sent), 1)
            rest = across(rest_part, far)
        arrived = exchange(sent, both)
        if first:
            down_bc = across(after(down_b, arrived), 1)
            rest_c = across(after(rest, arrived), 1)
            near = (up_weight, down_weight, up_c, down_c)
            distant = (up_a, up_b, down_a, down_b, rest, up_ac, up_bc, down_ac, down_bc, rest_c)
            sources = (total, ahead, behind, params, *near, *distant)
            total, sent, ups, downs = call(
                lambda *r: token_kernel(plan, True, False, *r),
                (
                    held,
                    wire,
                    jax.ShapeDtypeStruct((D, ch * up_weight.shape[1]), BF),
                    jax.ShapeDtypeStruct((ch * down_weight.shape[0], D), BF),
                ),
                (me, arrived, *sources),
                scratch
                + [pltpu.SemaphoreType.DMA((len(sources),))]
                + [pltpu.VMEM(t.shape, t.dtype) for t in sources[:4]],
                10**10,
                smem=1,
                far_in=len(sources),
                grant=24,
            )
            continue
        result = call(
            lambda *r: token_kernel(plan, False, last, *r),
            message if last else (held, wire),
            (arrived, total, ahead, behind, params, ups, downs),
            scratch,
            10**10,
        )
        if not last:
            total, sent = result
    result = exchange(result, "ch")
    result = call(
        lambda *r: unpack_kernel(plan, *r),
        jax.ShapeDtypeStruct((rows, width, wide), F32),
        (result,),
        [pltpu.VMEM((rows, width, LANES), F32)] * 2,
        10**8,
    )
    return result[None]


def solution(mesh):
    placed = (
        P(None, "lat", None, "ch"),
        P(None, "ch"),
        P(None, "ch"),
        P(None, "ch", None, None),
        P(None, "ch", None),
        P(None, "ch", None, None),
        P(None, "ch", None),
        P(None, "ch"),
        P("ch"),
        P("ch", None),
    )

    return jax.shard_map(
        local, mesh=mesh, in_specs=placed, out_specs=P(None, "lat", None, "ch"), check_vma=False
    )
```

```python
import math

import jax
import jax.numpy as jnp
import numpy as np
from jax import lax
from jax.experimental import pallas as pl
from jax.experimental.pallas import tpu as pltpu
from jax.sharding import PartitionSpec as P


D = 768
M = 64
STEPS = 4
EPS = 1e-05
SHRINK = 0.01
HALF = 64
PACK, START, FIRST = 24, 24, 58
LANES = 128
BF = jnp.bfloat16
F32 = jnp.float32


class Plan:
    def __init__(self, lat, ch, rows, width):
        self.lat, self.ch, self.rows, self.width = lat, ch, rows, width
        self.height = rows * lat
        self.short = width // ch
        self.padded = -(-self.short // 16) * 16
        self.tokens = rows * self.padded
        self.classes = self.short // 2 + 1
        self.per = -(-self.classes // lat)
        self.wide = D // ch
        self.units = self.wide // HALF
        self.items = rows * self.per
        spare = self.items % 8
        if self.items > 8 and spare and spare * self.units <= 8:
            self.main, self.left = self.items - spare, spare
        else:
            self.main, self.left = -(-self.items // 8) * 8, 0
        self.message = self.units * self.main + (8 if self.left else 0)
        slots = 0
        while (slots // 2) * self.short + (slots % 2) * (self.short - self.short // 2) < M:
            slots += 1
        self.slots = slots
        self.modes = self.per * slots * self.height
        self.peers = lat * ch
        self.spare = self.padded - self.short
        self.packed = self.tokens + self.tokens // 2
        hj = np.arange(self.main)
        self.item_h = np.where(hj < self.items, hj // self.per, 0)
        self.item_j = np.where(hj < self.items, hj % self.per, -1)
        tail = self.main + np.arange(self.left)
        self.tail_h, self.tail_j = tail // self.per, tail % self.per


def split_np(table):
    hi = table.astype(np.float32).astype(BF)
    lo = (table - hi.astype(np.float64)).astype(np.float32).astype(BF)
    return hi, lo


def short_tables(plan):
    g = np.arange(plan.lat)
    item_g = np.concatenate([np.repeat(g, plan.main), np.repeat(g, plan.left)])
    item_h = np.concatenate([np.tile(plan.item_h, plan.lat), np.tile(plan.tail_h, plan.lat)])
    item_j = np.concatenate([np.tile(plan.item_j, plan.lat), np.tile(plan.tail_j, plan.lat)])
    order = item_g * plan.per + item_j
    good = (item_j >= 0) & (order < plan.classes)
    tok_h = np.repeat(np.arange(plan.rows), plan.padded)
    tok_a = np.tile(np.arange(plan.padded), plan.rows)
    mask = good[:, None] & (item_h[:, None] == tok_h[None]) & (tok_a[None] < plan.short)
    angle = 2 * np.pi / plan.short * (order[:, None] * tok_a[None] % plan.short)
    cos, sin = np.cos(angle) * mask, np.sin(angle) * mask
    forward = np.concatenate([cos, -sin], 0)
    inverse = np.concatenate([cos.T, -sin.T], 1)
    side = max(forward.shape)
    tables = [np.pad(t, [(0, side - n) for n in t.shape]) for t in (forward, inverse)]
    return np.stack(split_np(tables[0]) + split_np(tables[1]))


def mode_places(plan):
    j, t, k = (
        v.reshape(-1)
        for v in np.meshgrid(
            np.arange(plan.per), np.arange(plan.slots), np.arange(plan.height), indexing="ij"
        )
    )
    peer = np.arange(plan.peers)
    col_p = np.concatenate([np.repeat(peer, plan.main), np.repeat(peer, plan.left)])
    col_h = np.concatenate([np.tile(plan.item_h, plan.peers), np.tile(plan.tail_h, plan.peers)])
    col_j = np.concatenate([np.tile(plan.item_j, plan.peers), np.tile(plan.tail_j, plan.peers)])
    col_h = (col_p // plan.ch) * plan.rows + col_h
    none = np.zeros_like(j)
    row = np.stack([j, t % 2, (t + 1) // 2, k] + [none] * 4).astype(np.float32)
    none = np.zeros_like(col_p)
    col = np.stack([col_p % plan.ch, col_h, col_j] + [none] * 5).astype(np.float32)
    return row, col


def cos_sin(turns):
    turns = turns - jnp.floor(turns + 0.5)
    quarter = jnp.floor(turns * 4.0 + 0.5)
    x = (turns - quarter * 0.25) * (2.0 * math.pi)
    y = x * x
    sin = x * (1 + y * (-1 / 6 + y * (1 / 120 + y * (-1 / 5040 + y * (1 / 362880)))))
    cos = 1 + y * (-0.5 + y * (1 / 24 + y * (-1 / 720 + y * (1 / 40320 - y * (1 / 3628800)))))
    odd = jnp.abs(quarter) == 1.0
    c, s = jnp.where(odd, sin, cos), jnp.where(odd, cos, sin)
    c = jnp.where((quarter == 1.0) | (jnp.abs(quarter) == 2.0), -c, c)
    s = jnp.where((quarter == -1.0) | (jnp.abs(quarter) == 2.0), -s, s)
    return c, s


def mode_table(plan, first_class, row, col):
    j, odd, times, k = row
    q, h, col_j = col
    order = first_class + j
    mode = times * plan.short + jnp.where(odd == 1.0, -order, order)
    fine = (mode < M) & (order < plan.classes)
    fine = fine & ((order > 0.0) | (times == 0.0) | (odd == 1.0))
    fine = fine & ((2.0 * order != plan.short) | (odd == 0.0))
    scale = 1.0 / math.sqrt(plan.height * plan.width)
    weight = jnp.where(fine, scale, 0.0)
    doubled = jnp.where(mode == 0.0, 1.0, 2.0)
    turn = jnp.where(odd == 1.0, 1.0, -1.0)
    product = k * h
    product = product - plan.height * jnp.floor(product * (1.0 / plan.height) + 1e-4)
    cos, sin = cos_sin(mode * q * (1.0 / plan.width) + product * (1.0 / plan.height))
    keep = jnp.where(j == col_j, weight, 0.0)
    return cos * keep, sin * (keep * turn), doubled


def split(value):
    hi = value.astype(BF)
    return hi, (value - hi.astype(F32)).astype(BF)


def dot(a, b):
    return jnp.dot(a, b, preferred_element_type=F32)


def low_lanes(shape):
    return lax.broadcasted_iota(jnp.int32, shape, len(shape) - 1) % LANES < HALF


def swap(value):
    return pltpu.roll(value, HALF, 1)


def norm(values, gain, shift):
    mean = jnp.sum(values, -1, keepdims=True) * (1.0 / D)
    spread = jnp.sum(values * values, -1, keepdims=True) * (1.0 / D) - mean * mean
    return (values - mean) * lax.rsqrt(spread + EPS) * gain + shift


def emit_wire(plan, normed, tab, wire_ref, scratch):
    hi, lo = split(normed)
    count = plan.lat * plan.main
    half = count + plan.lat * plan.left
    fhi, flo = tab[0, : 2 * half, : plan.tokens], tab[1, : 2 * half, : plan.tokens]
    spec = dot(fhi, hi) + dot(flo, hi) + dot(fhi, lo)
    low = low_lanes((half, LANES))
    for tile in range(D // LANES):
        lanes = slice(tile * LANES, (tile + 1) * LANES)
        re, im = spec[:half, lanes], spec[half:, lanes]
        pair = (jnp.where(low, re, swap(im)), jnp.where(low, swap(re), im))
        for which in range(2):
            c, u = divmod(2 * tile + which, plan.units)
            part = pair[which]
            scratch[:, c, u * plan.main : (u + 1) * plan.main, :] = part[:count].reshape(
                plan.lat, plan.main, LANES
            )
            for spot in range(plan.left):
                row = plan.units * plan.main + u * plan.left + spot
                for g in range(plan.lat):
                    at = count + g * plan.left + spot
                    scratch[g, c, row : row + 1, :] = part[at : at + 1]
    if plan.left:
        first = plan.units * (plan.main + plan.left)
        if first < plan.message:
            scratch[:, :, first:, :] = jnp.zeros(
                (plan.lat, plan.ch, plan.message - first, LANES), F32
            )
    wire_ref[...] = scratch[...].reshape(plan.peers, plan.message, LANES).astype(BF)


def read_wire(plan, wire_ref, tab, scratch):
    scratch[...] = wire_ref[...].astype(F32).reshape(plan.lat, plan.ch, plan.message, LANES)
    count = plan.lat * plan.main
    half = count + plan.lat * plan.left
    low = low_lanes((half, LANES))

    def unit(index):
        c, u = divmod(index, plan.units)
        parts = [scratch[:, c, u * plan.main : (u + 1) * plan.main, :].reshape(count, LANES)]
        for g in range(plan.lat):
            for spot in range(plan.left):
                row = plan.units * plan.main + u * plan.left + spot
                parts.append(scratch[g, c, row : row + 1, :])
        return jnp.concatenate(parts, 0) if len(parts) > 1 else parts[0]

    tiles = []
    for tile in range(D // LANES):
        a, b = unit(2 * tile), unit(2 * tile + 1)
        re = jnp.where(low, a, swap(b))
        im = jnp.where(low, swap(a), b)
        tiles.append(jnp.concatenate([re, im], 0).astype(BF))
    right = jnp.concatenate(tiles, 1)
    ghi, glo = tab[2, : plan.tokens, : 2 * half], tab[3, : plan.tokens, : 2 * half]
    return dot(ghi, right) + dot(glo, right)


def pack(values):
    half = values.shape[0] // 2
    tail = values[:, LANES:]
    return jnp.concatenate([values[:, :LANES], jnp.concatenate([tail[:half], tail[half:]], 1)], 0)


def unpack(message):
    tokens = message.shape[0] // 3 * 2
    tail = message[tokens:]
    tail = jnp.concatenate([tail[:, :HALF], tail[:, HALF:]], 0)
    return jnp.concatenate([message[:tokens], tail], 1)


def pack_kernel(plan, state_ref, gain_hbm, bias_hbm, up_hbm, out_ref, scratch, body, tail, *refs):
    gain_ref, bias_ref, up_ref, sem = refs
    copies = fetch([gain_hbm, bias_hbm, up_hbm], [gain_ref, bias_ref, up_ref], sem)
    body[...] = state_ref[:, :, :LANES]
    tail[:, :, :HALF] = state_ref[:, :, LANES:]
    for copy in copies:
        copy.wait()
    line = up_ref[...].astype(F32)
    small = [gain_ref[...].astype(F32), bias_ref[...].astype(F32)]
    small += [line[:, n * plan.wide : (n + 1) * plan.wide] for n in range(plan.ch)]
    small = jnp.concatenate(small, 0)
    count = small.shape[0]
    scratch[...] = jnp.zeros(scratch.shape, F32)
    for n in range(count):
        h, s = divmod(n, plan.spare)
        at = h * plan.padded + plan.short + s
        scratch[at : at + 1, :] = small[n : n + 1]
    for q in range(plan.ch):
        for h in range(plan.rows):
            at = h * plan.padded
            every = pl.ds(q, plan.short, stride=plan.ch)
            scratch[at : at + plan.short, :LANES] = body[h, every, :]
            scratch[at : at + plan.short, LANES:] = tail[h, every, :][:, :HALF]
        out_ref[q] = pack(scratch[...])


def unpack_kernel(plan, got_ref, out_ref, body, tail):
    for q in range(plan.ch):
        values = unpack(got_ref[q])
        wide = jnp.concatenate([values[:, LANES:], values[:, LANES:]], 1)
        for h in range(plan.rows):
            at = slice(h * plan.padded, h * plan.padded + plan.short)
            every = pl.ds(q, plan.short, stride=plan.ch)
            body[h, every, :] = values[at, :LANES]
            tail[h, every, :] = wide[at]
    out_ref[:, :, :LANES] = body[...]
    out_ref[:, :, LANES:] = tail[:, :, :HALF]


def fetch(sources, targets, sem):
    copies = [pltpu.make_async_copy(a, b, sem.at[n]) for n, (a, b) in enumerate(zip(sources, targets))]
    for copy in copies:
        copy.start()
    return copies


def parts_kernel(up_ref, down_ref, up_out, own_out, rest_out, *refs):
    mids, sem = refs[:3], refs[3]
    half, own = up_out.shape[1], own_out.shape[0]
    side = lax.axis_index("lat") % 2
    at = pl.multiple_of(side * half, LANES)
    to = pl.multiple_of(side * own, LANES)
    into = fetch(
        [up_ref.at[:, pl.ds(at, half)], down_ref.at[pl.ds(to, own), :], down_ref.at[2 * own :, :]],
        mids,
        sem,
    )
    away = []
    for n, out in enumerate((up_out, own_out, rest_out)):
        into[n].wait()
        away.append(pltpu.make_async_copy(mids[n], out, sem.at[3 + n]))
        away[n].start()
    for copy in away:
        copy.wait()


def table_kernel(plan, rowv, colv, rowt, colt, *refs):
    outs, (chi, clo, ehi, elo), sem = refs[:4], refs[4:8], refs[8]
    copies = [pltpu.make_async_copy(a, b, sem.at[n]) for n, (a, b) in enumerate(zip(refs[4:8], outs))]
    first = (lax.axis_index("lat") * plan.per).astype(F32)
    size = plan.modes
    wide = plan.peers * (plan.main + plan.left)
    rows = [rowv[:, n : n + 1] for n in range(4)]
    cols = [colv[n : n + 1, :] for n in range(3)]
    cos, sin, _ = mode_table(plan, first, rows, cols)
    chi[:, :wide], clo[:, :wide] = split(cos)
    chi[:, wide:], clo[:, wide:] = split(sin)
    copies[0].start()
    copies[1].start()
    rows = [rowt[n : n + 1, :] for n in range(4)]
    cols = [colt[:, n : n + 1] for n in range(3)]
    cos, sin, doubled = mode_table(plan, first, rows, cols)
    ehi[:, :size], elo[:, :size] = split(cos * doubled)
    ehi[:, size:], elo[:, size:] = split(-sin * doubled)
    copies[2].start()
    copies[3].start()
    for copy in copies:
        copy.wait()


def block_kernel(plan, fin, finb, fout, foutb, *refs):
    outs, (w1h, w1l, w2h, w2l, b1, b2), sem = refs[:6], refs[6:12], refs[12]
    copies = [pltpu.make_async_copy(a, b, sem.at[n]) for n, (a, b) in enumerate(zip(refs[6:12], outs))]
    for weights, bias, high, low, out in ((fin, finb, w1h, w1l, b1), (fout, foutb, w2h, w2l, b2)):
        blocks, channels = weights.shape[1], weights.shape[2]
        full = []
        for p in range(2):
            lines = []
            for n in range(blocks):
                cells = [jnp.zeros((channels, channels), F32)] * blocks
                cells[n] = weights[p, n]
                lines.append(jnp.concatenate(cells, 1))
            full.append(jnp.concatenate(lines, 0))
        for u in range(plan.units):
            at = slice(u * HALF, (u + 1) * HALF)
            real, imag = full[0][at], full[1][at]
            for p, (left, right) in enumerate(((real, imag), (-imag, real))):
                cells = []
                for v in range(plan.units):
                    cells += [left[:, v * HALF : (v + 1) * HALF], right[:, v * HALF : (v + 1) * HALF]]
                row = jnp.concatenate(cells, 1)
                to = slice((2 * u + p) * HALF, (2 * u + p + 1) * HALF)
                high[to, :], low[to, :] = split(row)
        lines = [jnp.concatenate([bias[p, n : n + 1] for n in range(blocks)], 1) for p in range(2)]
        cells = []
        for v in range(plan.units):
            cells += [line[:, v * HALF : (v + 1) * HALF] for line in lines]
        out[...] = jnp.concatenate(cells, 1)
    for copy in copies:
        copy.start()
    for copy in copies:
        copy.wait()


def start_kernel(plan, got_ref, tab_hbm, begun_hbm, wire_ref, *refs):
    scratch, tab, begun, sem = refs
    sum_ref, par_ref = begun.at[: plan.tokens], begun.at[plan.tokens :]
    bias_ref = par_ref.at[8:16]
    copies = fetch([tab_hbm], [tab], sem)
    got = [unpack(got_ref[c]) for c in range(plan.ch)]
    full = jnp.concatenate(got, 1)
    rows = []
    for h in range(plan.rows):
        for s in range(plan.spare):
            rows.append(h * plan.padded + plan.short + s)
    for n in range(5):
        par_ref[n : n + 1, :] = full[rows[n] : rows[n] + 1, :]
    par_ref[5:8, :] = jnp.zeros((3, D), F32)
    bias_ref[...] = jnp.zeros(bias_ref.shape, F32)
    for s in range(plan.ch):
        source = unpack(got_ref[lax.axis_index("ch") ^ s])
        parts = [source[rows[5 + n] : rows[5 + n] + 1, :] for n in range(plan.ch)]
        line = jnp.concatenate(parts, 1)
        bias_ref[s : s + 1, :] = line
    inside = lax.broadcasted_iota(jnp.int32, (plan.tokens, 1), 0) % plan.padded < plan.short
    values = jnp.where(inside, full, 0.0)
    normed = norm(values, par_ref[0:1, :], par_ref[2:3, :])
    sum_ref[...] = values + normed
    copies.append(pltpu.make_async_copy(begun, begun_hbm, sem.at[1]))
    copies[1].start()
    copies[0].wait()
    emit_wire(plan, normed, tab, wire_ref, scratch)
    copies[1].wait()


def token_kernel(plan, first, last, *refs):
    copies = []
    if first:
        wire_in, sources, refs = refs[0], refs[1:17], refs[17:]
        (sum_out, wire_out, par_out, up_all, down_all), refs = refs[:5], refs[5:]
        scratch, sem, (begun, tab) = refs[0], refs[1], refs[2:]
        sum_in, par_ref = begun.at[: plan.tokens], begun.at[plan.tokens :]
        shard = up_all.shape[1] // plan.ch
        half, own = shard // 2, shard // 6
        y = lax.axis_index("lat") % 2
        copies = fetch(sources[:2], (begun, tab), sem)
        groups = []
        weights = sources[2:]
        for s in range(plan.ch):
            at = s * shard
            if s < plan.ch // 2:
                ups, downs = weights[:1], weights[1:2]
                weights = weights[2:]
                ups = [(ups[0], up_all.at[:, at : at + shard])]
                downs = [(downs[0], down_all.at[at : at + shard, :])]
            else:
                ups, downs = weights[:2], weights[2:5]
                spots = [pl.multiple_of(at + n * half, LANES) for n in (y, 1 - y)]
                ups = [(w, up_all.at[:, pl.ds(n, half)]) for w, n in zip(ups, spots)]
                spots = [pl.multiple_of(at + n * own, LANES) for n in (y, 1 - y)]
                spots.append(at + 2 * own)
                sizes = (own, own, shard - 2 * own)
                downs = [
                    (w, down_all.at[pl.ds(n, size), :]) for w, n, size in zip(downs, spots, sizes)
                ]
                weights = weights[5:]
            group = []
            for source, target in ups + downs:
                count = len(copies)
                copies.append(pltpu.make_async_copy(source, target, sem.at[count]))
                copies[-1].start()
                group.append(copies[-1])
            groups.append(group)
        for copy in copies[:2]:
            copy.wait()
        par_out[...] = par_ref[...]
    else:
        wire_in, sum_in, tab, par_ref, up_all, down_all = refs[:6]
        outs, scratch = refs[6:-1], refs[-1]
        shard = up_all.shape[1] // plan.ch
        half = shard // 2
    values = sum_in[...] + read_wire(plan, wire_in, tab, scratch)
    normed = norm(values, par_ref[1:2, :], par_ref[3:4, :]).astype(BF)
    mixed = par_ref[4:5, :]
    for s in range(2 * plan.ch):
        if first and s % 2 == 0:
            for copy in groups[s // 2]:
                copy.wait()
        at = slice((s % 2) * half, (s % 2 + 1) * half)
        cut = slice(s * half, (s + 1) * half)
        bias = par_ref[8 + s // 2 : 9 + s // 2, at]
        pre = dot(normed, up_all[:, cut]) + bias
        hidden = (0.5 * pre * (1.0 + lax.erf(pre * math.sqrt(0.5)))).astype(BF)
        mixed = mixed + dot(hidden, down_all[cut, :])
    values = values + mixed
    if last:
        for c in range(plan.ch):
            outs[0][c] = pack(values[:, c * plan.wide : (c + 1) * plan.wide])
        return
    if not first:
        sum_out, wire_out = outs
    normed = norm(values, par_ref[0:1, :], par_ref[2:3, :])
    sum_out[...] = values + normed
    emit_wire(plan, normed, tab, wire_out, scratch)


def spectral_kernel(plan, far, wire_in, *refs):
    copies = []
    if far:
        sources, refs = refs[:11], refs[11:]
        wire_out, scratch, sem, mids = refs[0], refs[1], refs[2], refs[3:]
        copies = fetch(sources, mids, sem)
    else:
        mids, (wire_out, scratch) = refs[:11], refs[11:]
    chi, clo, ehi, elo, w1h, w1l, w2h, w2l, b1, b2, sign_ref = mids
    scratch[...] = wire_in[...].astype(F32)
    count = plan.peers * plan.main
    half = count + plan.peers * plan.left
    low = low_lanes((half, LANES))
    pieces = []
    for u in range(plan.units):
        parts = [scratch[:, u * plan.main : (u + 1) * plan.main, :].reshape(count, LANES)]
        for p in range(plan.peers if plan.left else 0):
            row = plan.units * plan.main + u * plan.left
            parts.append(scratch[p, row : row + plan.left, :])
        data = jnp.concatenate(parts, 0) if len(parts) > 1 else parts[0]
        turned = swap(data)
        turned = jnp.where(low, -turned, turned)
        pieces.append(jnp.concatenate([data, turned], 0).astype(BF))
    right = jnp.concatenate(pieces, 1)

    def ready(*which):
        for n in which if far else ():
            copies[n].wait()

    ready(0, 1, 10)
    spec = dot(chi[...], right) + dot(clo[...], right)
    sign = jnp.concatenate([sign_ref[...]] * plan.units, 1)
    spec = spec * sign

    def layer(value, wh, wl, bias):
        hi, lo = split(value)
        return dot(hi, wh[...]) + dot(hi, wl[...]) + dot(lo, wh[...]) + bias[...]

    ready(4, 5, 8)
    first = jnp.maximum(layer(spec, w1h, w1l, b1), 0.0)
    ready(6, 7, 9)
    second = layer(first, w2h, w2l, b2)
    shrunk = jnp.where(
        second > SHRINK, second - SHRINK, jnp.where(second < -SHRINK, second + SHRINK, 0.0)
    )
    shrunk = shrunk * sign
    low = low_lanes((plan.modes, LANES))
    pieces = []
    for u in range(plan.units):
        part = shrunk[:, u * LANES : (u + 1) * LANES]
        turned = swap(part)
        pieces.append(jnp.concatenate([part, jnp.where(low, -turned, turned)], 0))
    hi, lo = split(jnp.concatenate(pieces, 1))
    ready(2, 3)
    back = dot(ehi[...], hi) + dot(elo[...], hi) + dot(ehi[...], lo)
    for u in range(plan.units):
        part = back[:, u * LANES : (u + 1) * LANES]
        scratch[:, u * plan.main : (u + 1) * plan.main, :] = part[:count].reshape(
            plan.peers, plan.main, LANES
        )
        row = plan.units * plan.main + u * plan.left
        for p in range(plan.peers if plan.left else 0):
            at = count + p * plan.left
            scratch[p, row : row + plan.left, :] = part[at : at + plan.left]
    wire_out[...] = scratch[...].astype(BF)


def call(body, outs, operands, scratch, flops, far_in=0, far_out=(), grant=20):
    vmem = pl.BlockSpec(memory_space=pltpu.VMEM)
    anywhere = pl.BlockSpec(memory_space=pl.ANY)
    flat, tree = jax.tree.flatten(outs)
    out_specs = [anywhere if n in far_out else vmem for n in range(len(flat))]
    return pl.pallas_call(
        body,
        out_shape=outs,
        in_specs=[vmem] * (len(operands) - far_in) + [anywhere] * far_in,
        out_specs=jax.tree.unflatten(tree, out_specs),
        scratch_shapes=scratch,
        compiler_params=pltpu.CompilerParams(vmem_limit_bytes=grant * 2**20),
        cost_estimate=pl.CostEstimate(flops=flops, bytes_accessed=2**20, transcendentals=0),
    )(*operands)


def local(
    state,
    norm_gains,
    channel_biases,
    filter_in,
    filter_in_bias,
    filter_out,
    filter_out_bias,
    up_weight,
    up_bias,
    down_weight,
):
    _, rows, width, wide = state.shape
    plan = Plan(lax.axis_size("lat"), lax.axis_size("ch"), rows, width)
    ch = plan.ch
    far = ch // 2
    both = ("lat", "ch")
    assert plan.spare * rows >= 5 + ch and up_bias.shape[0] == ch * wide

    def across(value, step):
        return lax.ppermute(value, "ch", [(i, i ^ step) for i in range(ch)])

    def beside(value):
        return lax.ppermute(value, "lat", [(i, i ^ 1) for i in range(plan.lat)])

    def exchange(value, axes):
        return lax.all_to_all(value, axes, 0, 0, tiled=True)

    def after(value, token):
        return lax.optimization_barrier((value, token))[0]

    message = jax.ShapeDtypeStruct((ch, plan.packed, LANES), F32)
    tokens = call(
        lambda *r: pack_kernel(plan, *r),
        message,
        (state[0], norm_gains, channel_biases, up_bias.reshape(1, ch * wide)),
        [pltpu.VMEM((plan.tokens, wide), F32)]
        + [pltpu.VMEM((rows, width, LANES), F32)] * 2
        + [pltpu.VMEM(v.shape, BF) for v in (norm_gains, channel_biases, up_bias.reshape(1, -1))]
        + [pltpu.SemaphoreType.DMA((3,))],
        10**8,
        far_in=3,
        grant=PACK,
    )
    got = exchange(tokens, "ch")

    half, own = up_weight.shape[1] // 2, down_weight.shape[0] // 6
    shapes = [(D, half), (own, D), (down_weight.shape[0] - 2 * own, D)]
    parts = [jax.ShapeDtypeStruct(shape, BF) for shape in shapes]
    up_part, own_part, rest_part = call(
        parts_kernel,
        tuple(parts),
        (up_weight, down_weight),
        [pltpu.VMEM(t.shape, BF) for t in parts] + [pltpu.SemaphoreType.DMA((6,))],
        10**6,
        far_in=2,
        far_out=(0, 1, 2),
        grant=58,
    )
    up_a = across(up_part, far)
    blocks = [jax.ShapeDtypeStruct((2 * wide, 2 * wide), BF)] * 4
    blocks += [jax.ShapeDtypeStruct((1, 2 * wide), F32)] * 2
    blocks = call(
        lambda *r: block_kernel(plan, *r),
        tuple(blocks),
        (filter_in, filter_in_bias, filter_out, filter_out_bias),
        [pltpu.VMEM(t.shape, t.dtype) for t in blocks] + [pltpu.SemaphoreType.DMA((6,))],
        10**8,
        far_out=range(6),
        grant=58,
    )
    got, *blocks = lax.optimization_barrier((got, *blocks))
    up_c, down_c = across(up_weight, 1), across(down_weight, 1)

    short = jnp.asarray(short_tables(plan))
    odd = np.tile(np.repeat(np.arange(plan.slots) % 2, plan.height), plan.per)
    sign = np.where((odd[:, None] == 1) & (np.arange(LANES)[None] >= HALF), -1.0, 1.0)
    sign = sign.astype(np.float32)

    wire = jax.ShapeDtypeStruct((plan.peers, plan.message, LANES), BF)
    held = jax.ShapeDtypeStruct((plan.tokens, D), F32)
    scratch = [pltpu.VMEM((plan.lat, ch, plan.message, LANES), F32)]
    begun = jax.ShapeDtypeStruct((plan.tokens + 16, D), F32)
    begun, sent = call(
        lambda *r: start_kernel(plan, *r),
        (begun, wire),
        (got, short),
        scratch
        + [pltpu.VMEM(t.shape, t.dtype) for t in (short, begun)]
        + [pltpu.SemaphoreType.DMA((2,))],
        10**9,
        far_in=1,
        far_out=(0,),
        grant=START,
    )
    row, col = mode_places(plan)
    lines = plan.peers * (plan.main + plan.left)
    dims = [(plan.modes, 2 * lines)] * 2 + [(lines, 2 * plan.modes)] * 2
    tables = [jax.ShapeDtypeStruct(shape, BF) for shape in dims]
    made = call(
        lambda *r: table_kernel(plan, *r),
        tuple(tables),
        (after(jnp.asarray(row.T), sent), col, row, col.T),
        [pltpu.VMEM(t.shape, t.dtype) for t in tables] + [pltpu.SemaphoreType.DMA((4,))],
        10**8,
        far_out=range(4),
        grant=58,
    )
    spectral_in = (*made, *blocks)
    for step_index in range(STEPS):
        first, last = step_index == 0, step_index == STEPS - 1
        arrived = exchange(sent, both)
        if first:
            down_a = across(own_part, far)
            rest = across(rest_part, far)
            up_b = beside(up_a)
            up_ac = across(up_a, 1)
        tabs = (*spectral_in, sign)
        mids = [pltpu.VMEM(t.shape, t.dtype) for t in tabs] if first else []
        sent = call(
            lambda *r: spectral_kernel(plan, first, *r),
            wire,
            (arrived, *tabs),
            [pltpu.VMEM((plan.peers, plan.message, LANES), F32)]
            + ([pltpu.SemaphoreType.DMA((len(tabs),))] if first else [])
            + mids,
            10**9,
            far_in=len(mids),
            grant=FIRST if first else 20,
        )
        if first:
            up_bc = across(after(up_b, sent), 1)
            down_b = beside(after(down_a, sent))
            down_ac = across(after(down_a, sent), 1)
            rest_c = across(after(rest, sent), 1)
        arrived = exchange(sent, both)
        if first:
            down_bc = across(after(down_b, arrived), 1)
            near = (up_weight, down_weight, up_c, down_c)
            distant = (up_a, up_b, down_a, down_b, rest, up_ac, up_bc, down_ac, down_bc, rest_c)
            sources = (begun, short, *near, *distant)
            total, sent, params, ups, downs = call(
                lambda *r: token_kernel(plan, True, False, *r),
                (
                    held,
                    wire,
                    jax.ShapeDtypeStruct((16, D), F32),
                    jax.ShapeDtypeStruct((D, ch * up_weight.shape[1]), BF),
                    jax.ShapeDtypeStruct((ch * down_weight.shape[0], D), BF),
                ),
                (arrived, *sources),
                scratch
                + [pltpu.SemaphoreType.DMA((len(sources),))]
                + [pltpu.VMEM(t.shape, t.dtype) for t in sources[:2]],
                10**10,
                        far_in=len(sources),
                grant=24,
            )
            continue
        result = call(
            lambda *r: token_kernel(plan, False, last, *r),
            message if last else (held, wire),
            (arrived, total, short, params, ups, downs),
            scratch,
            10**10,
        )
        if not last:
            total, sent = result
    result = exchange(result, "ch")
    result = call(
        lambda *r: unpack_kernel(plan, *r),
        jax.ShapeDtypeStruct((rows, width, wide), F32),
        (result,),
        [pltpu.VMEM((rows, width, LANES), F32)] * 2,
        10**8,
    )
    return result[None]


def solution(mesh):
    placed = (
        P(None, "lat", None, "ch"),
        P(None, "ch"),
        P(None, "ch"),
        P(None, "ch", None, None),
        P(None, "ch", None),
        P(None, "ch", None, None),
        P(None, "ch", None),
        P(None, "ch"),
        P("ch"),
        P("ch", None),
    )

    return jax.shard_map(
        local, mesh=mesh, in_specs=placed, out_specs=P(None, "lat", None, "ch"), check_vma=False
    )
```

```python
import math

import jax
import jax.numpy as jnp
import numpy as np
from jax import lax
from jax.experimental import pallas as pl
from jax.experimental.pallas import tpu as pltpu
from jax.sharding import PartitionSpec as P


D = 768
M = 64
STEPS = 4
EPS = 1e-05
SHRINK = 0.01
HALF = 64
PACK, START, FIRST = 24, 24, 58
PART = 4
LANES = 128
BF = jnp.bfloat16
F32 = jnp.float32


class Plan:
    def __init__(self, lat, ch, rows, width):
        self.lat, self.ch, self.rows, self.width = lat, ch, rows, width
        self.height = rows * lat
        self.short = width // ch
        self.padded = -(-self.short // 16) * 16
        self.tokens = rows * self.padded
        self.classes = self.short // 2 + 1
        self.per = -(-self.classes // lat)
        self.wide = D // ch
        self.units = self.wide // HALF
        self.items = rows * self.per
        spare = self.items % 8
        if self.items > 8 and spare and spare * self.units <= 8:
            self.main, self.left = self.items - spare, spare
        else:
            self.main, self.left = -(-self.items // 8) * 8, 0
        self.message = self.units * self.main + (8 if self.left else 0)
        slots = 0
        while (slots // 2) * self.short + (slots % 2) * (self.short - self.short // 2) < M:
            slots += 1
        self.slots = slots
        self.modes = self.per * slots * self.height
        self.peers = lat * ch
        self.spare = self.padded - self.short
        self.packed = self.tokens + self.tokens // 2
        hj = np.arange(self.main)
        self.item_h = np.where(hj < self.items, hj // self.per, 0)
        self.item_j = np.where(hj < self.items, hj % self.per, -1)
        tail = self.main + np.arange(self.left)
        self.tail_h, self.tail_j = tail // self.per, tail % self.per


def split_np(table):
    hi = table.astype(np.float32).astype(BF)
    lo = (table - hi.astype(np.float64)).astype(np.float32).astype(BF)
    return hi, lo


def short_tables(plan):
    g = np.arange(plan.lat)
    item_g = np.concatenate([np.repeat(g, plan.main), np.repeat(g, plan.left)])
    item_h = np.concatenate([np.tile(plan.item_h, plan.lat), np.tile(plan.tail_h, plan.lat)])
    item_j = np.concatenate([np.tile(plan.item_j, plan.lat), np.tile(plan.tail_j, plan.lat)])
    order = item_g * plan.per + item_j
    good = (item_j >= 0) & (order < plan.classes)
    tok_h = np.repeat(np.arange(plan.rows), plan.padded)
    tok_a = np.tile(np.arange(plan.padded), plan.rows)
    mask = good[:, None] & (item_h[:, None] == tok_h[None]) & (tok_a[None] < plan.short)
    angle = 2 * np.pi / plan.short * (order[:, None] * tok_a[None] % plan.short)
    cos, sin = np.cos(angle) * mask, np.sin(angle) * mask
    forward = np.concatenate([cos, -sin], 0)
    inverse = np.concatenate([cos.T, -sin.T], 1)
    side = max(forward.shape)
    tables = [np.pad(t, [(0, side - n) for n in t.shape]) for t in (forward, inverse)]
    return np.stack(split_np(tables[0]) + split_np(tables[1]))


def mode_places(plan):
    j, t, k = (
        v.reshape(-1)
        for v in np.meshgrid(
            np.arange(plan.per), np.arange(plan.slots), np.arange(plan.height), indexing="ij"
        )
    )
    peer = np.arange(plan.peers)
    col_p = np.concatenate([np.repeat(peer, plan.main), np.repeat(peer, plan.left)])
    col_h = np.concatenate([np.tile(plan.item_h, plan.peers), np.tile(plan.tail_h, plan.peers)])
    col_j = np.concatenate([np.tile(plan.item_j, plan.peers), np.tile(plan.tail_j, plan.peers)])
    col_h = (col_p // plan.ch) * plan.rows + col_h
    none = np.zeros_like(j)
    row = np.stack([j, t % 2, (t + 1) // 2, k] + [none] * 4).astype(np.float32)
    none = np.zeros_like(col_p)
    col = np.stack([col_p % plan.ch, col_h, col_j] + [none] * 5).astype(np.float32)
    return row, col


def cos_sin(turns):
    turns = turns - jnp.floor(turns + 0.5)
    quarter = jnp.floor(turns * 4.0 + 0.5)
    x = (turns - quarter * 0.25) * (2.0 * math.pi)
    y = x * x
    sin = x * (1 + y * (-1 / 6 + y * (1 / 120 + y * (-1 / 5040 + y * (1 / 362880)))))
    cos = 1 + y * (-0.5 + y * (1 / 24 + y * (-1 / 720 + y * (1 / 40320 - y * (1 / 3628800)))))
    odd = jnp.abs(quarter) == 1.0
    c, s = jnp.where(odd, sin, cos), jnp.where(odd, cos, sin)
    c = jnp.where((quarter == 1.0) | (jnp.abs(quarter) == 2.0), -c, c)
    s = jnp.where((quarter == -1.0) | (jnp.abs(quarter) == 2.0), -s, s)
    return c, s


def mode_table(plan, first_class, row, col):
    j, odd, times, k = row
    q, h, col_j = col
    order = first_class + j
    mode = times * plan.short + jnp.where(odd == 1.0, -order, order)
    fine = (mode < M) & (order < plan.classes)
    fine = fine & ((order > 0.0) | (times == 0.0) | (odd == 1.0))
    fine = fine & ((2.0 * order != plan.short) | (odd == 0.0))
    scale = 1.0 / math.sqrt(plan.height * plan.width)
    weight = jnp.where(fine, scale, 0.0)
    doubled = jnp.where(mode == 0.0, 1.0, 2.0)
    turn = jnp.where(odd == 1.0, 1.0, -1.0)
    product = k * h
    product = product - plan.height * jnp.floor(product * (1.0 / plan.height) + 1e-4)
    cos, sin = cos_sin(mode * q * (1.0 / plan.width) + product * (1.0 / plan.height))
    keep = jnp.where(j == col_j, weight, 0.0)
    return cos * keep, sin * (keep * turn), doubled


def split(value):
    hi = value.astype(BF)
    return hi, (value - hi.astype(F32)).astype(BF)


def dot(a, b):
    return jnp.dot(a, b, preferred_element_type=F32)


def low_lanes(shape):
    return lax.broadcasted_iota(jnp.int32, shape, len(shape) - 1) % LANES < HALF


def swap(value):
    return pltpu.roll(value, HALF, 1)


def norm(values, gain, shift):
    mean = jnp.sum(values, -1, keepdims=True) * (1.0 / D)
    spread = jnp.sum(values * values, -1, keepdims=True) * (1.0 / D) - mean * mean
    return (values - mean) * lax.rsqrt(spread + EPS) * gain + shift


def emit_wire(plan, normed, tab, wire_ref, scratch):
    hi, lo = split(normed)
    count = plan.lat * plan.main
    half = count + plan.lat * plan.left
    fhi, flo = tab[0, : 2 * half, : plan.tokens], tab[1, : 2 * half, : plan.tokens]
    spec = dot(fhi, hi) + dot(flo, hi) + dot(fhi, lo)
    low = low_lanes((half, LANES))
    for tile in range(D // LANES):
        lanes = slice(tile * LANES, (tile + 1) * LANES)
        re, im = spec[:half, lanes], spec[half:, lanes]
        pair = (jnp.where(low, re, swap(im)), jnp.where(low, swap(re), im))
        for which in range(2):
            c, u = divmod(2 * tile + which, plan.units)
            part = pair[which]
            scratch[:, c, u * plan.main : (u + 1) * plan.main, :] = part[:count].reshape(
                plan.lat, plan.main, LANES
            )
            for spot in range(plan.left):
                row = plan.units * plan.main + u * plan.left + spot
                for g in range(plan.lat):
                    at = count + g * plan.left + spot
                    scratch[g, c, row : row + 1, :] = part[at : at + 1]
    if plan.left:
        first = plan.units * (plan.main + plan.left)
        if first < plan.message:
            scratch[:, :, first:, :] = jnp.zeros(
                (plan.lat, plan.ch, plan.message - first, LANES), F32
            )
    wire_ref[...] = scratch[...].reshape(plan.peers, plan.message, LANES).astype(BF)


def read_wire(plan, wire_ref, tab, scratch):
    scratch[...] = wire_ref[...].astype(F32).reshape(plan.lat, plan.ch, plan.message, LANES)
    count = plan.lat * plan.main
    half = count + plan.lat * plan.left
    low = low_lanes((half, LANES))

    def unit(index):
        c, u = divmod(index, plan.units)
        parts = [scratch[:, c, u * plan.main : (u + 1) * plan.main, :].reshape(count, LANES)]
        for g in range(plan.lat):
            for spot in range(plan.left):
                row = plan.units * plan.main + u * plan.left + spot
                parts.append(scratch[g, c, row : row + 1, :])
        return jnp.concatenate(parts, 0) if len(parts) > 1 else parts[0]

    tiles = []
    for tile in range(D // LANES):
        a, b = unit(2 * tile), unit(2 * tile + 1)
        re = jnp.where(low, a, swap(b))
        im = jnp.where(low, swap(a), b)
        tiles.append(jnp.concatenate([re, im], 0).astype(BF))
    right = jnp.concatenate(tiles, 1)
    ghi, glo = tab[2, : plan.tokens, : 2 * half], tab[3, : plan.tokens, : 2 * half]
    return dot(ghi, right) + dot(glo, right)


def pack(values):
    half = values.shape[0] // 2
    tail = values[:, LANES:]
    return jnp.concatenate([values[:, :LANES], jnp.concatenate([tail[:half], tail[half:]], 1)], 0)


def unpack(message):
    tokens = message.shape[0] // 3 * 2
    tail = message[tokens:]
    tail = jnp.concatenate([tail[:, :HALF], tail[:, HALF:]], 0)
    return jnp.concatenate([message[:tokens], tail], 1)


def pack_kernel(plan, state_ref, gain_hbm, bias_hbm, up_hbm, out_ref, scratch, body, tail, *refs):
    gain_ref, bias_ref, up_ref, sem = refs
    copies = fetch([gain_hbm, bias_hbm, up_hbm], [gain_ref, bias_ref, up_ref], sem)
    body[...] = state_ref[:, :, :LANES]
    tail[:, :, :HALF] = state_ref[:, :, LANES:]
    for copy in copies:
        copy.wait()
    line = up_ref[...].astype(F32)
    small = [gain_ref[...].astype(F32), bias_ref[...].astype(F32)]
    small += [line[:, n * plan.wide : (n + 1) * plan.wide] for n in range(plan.ch)]
    small = jnp.concatenate(small, 0)
    count = small.shape[0]
    scratch[...] = jnp.zeros(scratch.shape, F32)
    for n in range(count):
        h, s = divmod(n, plan.spare)
        at = h * plan.padded + plan.short + s
        scratch[at : at + 1, :] = small[n : n + 1]
    for q in range(plan.ch):
        for h in range(plan.rows):
            at = h * plan.padded
            every = pl.ds(q, plan.short, stride=plan.ch)
            scratch[at : at + plan.short, :LANES] = body[h, every, :]
            scratch[at : at + plan.short, LANES:] = tail[h, every, :][:, :HALF]
        out_ref[q] = pack(scratch[...])


def unpack_kernel(plan, got_ref, out_ref, body, tail):
    for q in range(plan.ch):
        values = unpack(got_ref[q])
        wide = jnp.concatenate([values[:, LANES:], values[:, LANES:]], 1)
        for h in range(plan.rows):
            at = slice(h * plan.padded, h * plan.padded + plan.short)
            every = pl.ds(q, plan.short, stride=plan.ch)
            body[h, every, :] = values[at, :LANES]
            tail[h, every, :] = wide[at]
    out_ref[:, :, :LANES] = body[...]
    out_ref[:, :, LANES:] = tail[:, :, :HALF]


def fetch(sources, targets, sem):
    copies = [pltpu.make_async_copy(a, b, sem.at[n]) for n, (a, b) in enumerate(zip(sources, targets))]
    for copy in copies:
        copy.start()
    return copies


def parts_kernel(up_ref, down_ref, up_out, own_out, rest_out, *refs):
    mids, sem = refs[:3], refs[3]
    half, own = up_out.shape[1], own_out.shape[0]
    side = lax.axis_index("lat") % 2
    at = pl.multiple_of(side * half, LANES)
    to = pl.multiple_of(side * own, HALF)
    into = fetch(
        [up_ref.at[:, pl.ds(at, half)], down_ref.at[pl.ds(to, own), :], down_ref.at[2 * own :, :]],
        mids,
        sem,
    )
    away = []
    for n, out in enumerate((up_out, own_out, rest_out)):
        into[n].wait()
        away.append(pltpu.make_async_copy(mids[n], out, sem.at[3 + n]))
        away[n].start()
    for copy in away:
        copy.wait()


def fill_tables(plan, rowv, colv, rowt, colt, chi, clo, ehi, elo):
    first = (lax.axis_index("lat") * plan.per).astype(F32)
    size = plan.modes
    wide = plan.peers * (plan.main + plan.left)
    rows = [rowv[:, n : n + 1] for n in range(4)]
    cols = [colv[n : n + 1, :] for n in range(3)]
    cos, sin, _ = mode_table(plan, first, rows, cols)
    chi[:, :wide], clo[:, :wide] = split(cos)
    chi[:, wide:], clo[:, wide:] = split(sin)
    rows = [rowt[n : n + 1, :] for n in range(4)]
    cols = [colt[:, n : n + 1] for n in range(3)]
    cos, sin, doubled = mode_table(plan, first, rows, cols)
    ehi[:, :size], elo[:, :size] = split(cos * doubled)
    ehi[:, size:], elo[:, size:] = split(-sin * doubled)


def high_units(plan):
    return plan.units - 1


def block_kernel(plan, fin, finb, fout, foutb, *refs):
    outs, (w1h, w1l, w2h, w2l, b1, b2), sem = refs[:6], refs[6:12], refs[12]
    copies = [pltpu.make_async_copy(a, b, sem.at[n]) for n, (a, b) in enumerate(zip(refs[6:12], outs))]
    span = high_units(plan)
    for weights, bias, high, low, out in ((fin, finb, w1h, w1l, b1), (fout, foutb, w2h, w2l, b2)):
        blocks, channels = weights.shape[1], weights.shape[2]
        for n in range(blocks):
            full = []
            for p in range(2):
                lines = [jnp.zeros((channels, blocks * channels), F32)] * blocks
                cells = [jnp.zeros((channels, channels), F32)] * blocks
                cells[n] = weights[p, n]
                lines[n] = jnp.concatenate(cells, 1)
                full.append(jnp.concatenate(lines, 0))
            for u in range(n, n + span):
                at = slice(u * HALF, (u + 1) * HALF)
                real, imag = full[0][at], full[1][at]
                for p, (left, right) in enumerate(((real, imag), (-imag, real))):
                    cells = []
                    for v in range(n, n + span):
                        cut = slice(v * HALF, (v + 1) * HALF)
                        cells += [left[:, cut], right[:, cut]]
                    row = jnp.concatenate(cells, 1)
                    to = slice((2 * (u - n) + p) * HALF, (2 * (u - n) + p + 1) * HALF)
                    high[n, to, :], low[n, to, :] = split(row)
        lines = [jnp.concatenate([bias[p, n : n + 1] for n in range(blocks)], 1) for p in range(2)]
        cells = []
        for v in range(plan.units):
            cells += [line[:, v * HALF : (v + 1) * HALF] for line in lines]
        out[...] = jnp.concatenate(cells, 1)
    for copy in copies:
        copy.start()
    for copy in copies:
        copy.wait()


def start_kernel(plan, got_ref, tab_hbm, begun_hbm, wire_ref, *refs):
    scratch, tab, begun, sem = refs
    sum_ref, par_ref = begun.at[: plan.tokens], begun.at[plan.tokens : plan.tokens + 16]
    bias_ref = par_ref.at[8:16]
    copies = fetch([tab_hbm], [tab], sem)
    got = [unpack(got_ref[c]) for c in range(plan.ch)]
    full = jnp.concatenate(got, 1)
    rows = []
    for h in range(plan.rows):
        for s in range(plan.spare):
            rows.append(h * plan.padded + plan.short + s)
    for n in range(5):
        par_ref[n : n + 1, :] = full[rows[n] : rows[n] + 1, :]
    par_ref[5:8, :] = jnp.zeros((3, D), F32)
    bias_ref[...] = jnp.zeros(bias_ref.shape, F32)
    for s in range(plan.ch):
        source = unpack(got_ref[lax.axis_index("ch") ^ s])
        parts = [source[rows[5 + n] : rows[5 + n] + 1, :] for n in range(plan.ch)]
        line = jnp.concatenate(parts, 1)
        bias_ref[s : s + 1, :] = line
    inside = lax.broadcasted_iota(jnp.int32, (plan.tokens, 1), 0) % plan.padded < plan.short
    values = jnp.where(inside, full, 0.0)
    normed = norm(values, par_ref[0:1, :], par_ref[2:3, :])
    sum_ref[...] = values + normed
    copies[0].wait()
    side = tab.shape[1]
    rows = slice(plan.tokens + 16, plan.tokens + 16 + side)
    for n in range(2):
        whole = tab[2 * n].astype(F32) + tab[2 * n + 1].astype(F32)
        begun[rows, 256 * n : 256 * n + side] = whole
    copies.append(pltpu.make_async_copy(begun, begun_hbm, sem.at[1]))
    copies[1].start()
    emit_wire(plan, normed, tab, wire_ref, scratch)
    copies[1].wait()


def token_kernel(plan, first, last, *refs):
    copies = []
    if first:
        wire_in, sources, refs = refs[0], refs[1:16], refs[16:]
        (sum_out, wire_out, par_out, up_all, down_all), refs = refs[:5], refs[5:]
        scratch, sem, (begun, tab) = refs[0], refs[1], refs[2:]
        sum_in, par_ref = begun.at[: plan.tokens], begun.at[plan.tokens : plan.tokens + 16]
        shard = up_all.shape[1] // plan.ch
        half, own = shard // 2, shard // PART
        y = lax.axis_index("lat") % 2
        copies = fetch(sources[:1], (begun,), sem)
        groups = []
        weights = sources[1:]
        for s in range(plan.ch):
            at = s * shard
            if s < plan.ch // 2:
                ups, downs = weights[:1], weights[1:2]
                weights = weights[2:]
                ups = [(ups[0], up_all.at[:, at : at + shard])]
                downs = [(downs[0], down_all.at[at : at + shard, :])]
            else:
                ups, downs = weights[:2], weights[2:5]
                spots = [pl.multiple_of(at + n * half, LANES) for n in (y, 1 - y)]
                ups = [(w, up_all.at[:, pl.ds(n, half)]) for w, n in zip(ups, spots)]
                spots = [pl.multiple_of(at + n * own, HALF) for n in (y, 1 - y)]
                spots.append(at + 2 * own)
                sizes = (own, own, shard - 2 * own)
                downs = [
                    (w, down_all.at[pl.ds(n, size), :]) for w, n, size in zip(downs, spots, sizes)
                ]
                weights = weights[5:]
            group = []
            for source, target in ups + downs:
                count = len(copies)
                copies.append(pltpu.make_async_copy(source, target, sem.at[count]))
                copies[-1].start()
                group.append(copies[-1])
            groups.append(group)
        copies[0].wait()
        side = tab.shape[1]
        for n in range(2):
            whole = begun[plan.tokens + 16 :, 256 * n : 256 * n + side]
            tab[2 * n], tab[2 * n + 1] = split(whole)
        par_out[...] = par_ref[...]
    else:
        wire_in, sum_in, tab, par_ref, up_all, down_all = refs[:6]
        outs, scratch = refs[6:-1], refs[-1]
        shard = up_all.shape[1] // plan.ch
        half = shard // 2
    values = sum_in[...] + read_wire(plan, wire_in, tab, scratch)
    normed = norm(values, par_ref[1:2, :], par_ref[3:4, :]).astype(BF)
    mixed = par_ref[4:5, :]
    for s in range(2 * plan.ch):
        if first and s % 2 == 0:
            for copy in groups[s // 2]:
                copy.wait()
        at = slice((s % 2) * half, (s % 2 + 1) * half)
        cut = slice(s * half, (s + 1) * half)
        bias = par_ref[8 + s // 2 : 9 + s // 2, at]
        pre = dot(normed, up_all[:, cut]) + bias
        hidden = (0.5 * pre * (1.0 + lax.erf(pre * math.sqrt(0.5)))).astype(BF)
        mixed = mixed + dot(hidden, down_all[cut, :])
    values = values + mixed
    if last:
        for c in range(plan.ch):
            outs[0][c] = pack(values[:, c * plan.wide : (c + 1) * plan.wide])
        return
    if not first:
        sum_out, wire_out = outs
    normed = norm(values, par_ref[0:1, :], par_ref[2:3, :])
    sum_out[...] = values + normed
    emit_wire(plan, normed, tab, wire_out, scratch)


def spectral_kernel(plan, far, wire_in, *refs):
    copies, away = [], []
    if far:
        places, sign_ref, sources, wire_out = refs[:4], refs[4], refs[5:11], refs[11]
        outs, scratch, sem = refs[12:16], refs[16], refs[17]
        chi, clo, ehi, elo = tables = refs[18:22]
        w1h, w1l, w2h, w2l, b1, b2 = mids = refs[22:]
        copies = fetch(sources, mids, sem)
        fill_tables(plan, *places, *tables)
        for n, (table, out) in enumerate(zip(tables, outs)):
            away.append(pltpu.make_async_copy(table, out, sem.at[6 + n]))
            away[n].start()
    else:
        chi, clo, ehi, elo, w1h, w1l, w2h, w2l, b1, b2, sign_ref, wire_out, scratch = refs
    scratch[...] = wire_in[...].astype(F32)
    count = plan.peers * plan.main
    half = count + plan.peers * plan.left
    low = low_lanes((half, LANES))
    pieces = []
    for u in range(plan.units):
        parts = [scratch[:, u * plan.main : (u + 1) * plan.main, :].reshape(count, LANES)]
        for p in range(plan.peers if plan.left else 0):
            row = plan.units * plan.main + u * plan.left
            parts.append(scratch[p, row : row + plan.left, :])
        data = jnp.concatenate(parts, 0) if len(parts) > 1 else parts[0]
        turned = swap(data)
        turned = jnp.where(low, -turned, turned)
        pieces.append(jnp.concatenate([data, turned], 0).astype(BF))
    right = jnp.concatenate(pieces, 1)

    def ready(*which):
        for n in which if far else ():
            copies[n].wait()

    spec = dot(chi[...], right) + dot(clo[...], right)
    sign = jnp.concatenate([sign_ref[...]] * plan.units, 1)
    spec = spec * sign

    def layer(value, wh, wl, bias):
        hi, lo = split(value)
        span, total = wh.shape[1], 0.0
        for n in range(wh.shape[0]):
            cut = slice(n * LANES, n * LANES + span)
            part = dot(hi[:, cut], wh[n]) + dot(hi[:, cut], wl[n]) + dot(lo[:, cut], wh[n])
            sides = [(part.shape[0], n * LANES), (part.shape[0], value.shape[1] - span - n * LANES)]
            cells = [jnp.zeros(sides[0], F32)] * (n > 0) + [part]
            cells += [jnp.zeros(sides[1], F32)] * (sides[1][1] > 0)
            total = total + jnp.concatenate(cells, 1)
        return total + bias[...]

    ready(0, 1, 4)
    first = jnp.maximum(layer(spec, w1h, w1l, b1), 0.0)
    ready(2, 3, 5)
    second = layer(first, w2h, w2l, b2)
    shrunk = jnp.where(
        second > SHRINK, second - SHRINK, jnp.where(second < -SHRINK, second + SHRINK, 0.0)
    )
    shrunk = shrunk * sign
    low = low_lanes((plan.modes, LANES))
    pieces = []
    for u in range(plan.units):
        part = shrunk[:, u * LANES : (u + 1) * LANES]
        turned = swap(part)
        pieces.append(jnp.concatenate([part, jnp.where(low, -turned, turned)], 0))
    hi, lo = split(jnp.concatenate(pieces, 1))
    back = dot(ehi[...], hi) + dot(elo[...], hi) + dot(ehi[...], lo)
    for u in range(plan.units):
        part = back[:, u * LANES : (u + 1) * LANES]
        scratch[:, u * plan.main : (u + 1) * plan.main, :] = part[:count].reshape(
            plan.peers, plan.main, LANES
        )
        row = plan.units * plan.main + u * plan.left
        for p in range(plan.peers if plan.left else 0):
            at = count + p * plan.left
            scratch[p, row : row + plan.left, :] = part[at : at + plan.left]
    wire_out[...] = scratch[...].astype(BF)
    for copy in away:
        copy.wait()


def call(body, outs, operands, scratch, flops, far_in=0, far_out=(), grant=20):
    vmem = pl.BlockSpec(memory_space=pltpu.VMEM)
    anywhere = pl.BlockSpec(memory_space=pl.ANY)
    flat, tree = jax.tree.flatten(outs)
    out_specs = [anywhere if n in far_out else vmem for n in range(len(flat))]
    return pl.pallas_call(
        body,
        out_shape=outs,
        in_specs=[vmem] * (len(operands) - far_in) + [anywhere] * far_in,
        out_specs=jax.tree.unflatten(tree, out_specs),
        scratch_shapes=scratch,
        compiler_params=pltpu.CompilerParams(vmem_limit_bytes=grant * 2**20),
        cost_estimate=pl.CostEstimate(flops=flops, bytes_accessed=2**20, transcendentals=0),
    )(*operands)


def local(
    state,
    norm_gains,
    channel_biases,
    filter_in,
    filter_in_bias,
    filter_out,
    filter_out_bias,
    up_weight,
    up_bias,
    down_weight,
):
    _, rows, width, wide = state.shape
    plan = Plan(lax.axis_size("lat"), lax.axis_size("ch"), rows, width)
    ch = plan.ch
    far = ch // 2
    both = ("lat", "ch")
    assert plan.spare * rows >= 5 + ch and up_bias.shape[0] == ch * wide

    def across(value, step):
        return lax.ppermute(value, "ch", [(i, i ^ step) for i in range(ch)])

    def beside(value):
        return lax.ppermute(value, "lat", [(i, i ^ 1) for i in range(plan.lat)])

    def exchange(value, axes):
        return lax.all_to_all(value, axes, 0, 0, tiled=True)

    def after(value, token):
        return lax.optimization_barrier((value, token))[0]

    message = jax.ShapeDtypeStruct((ch, plan.packed, LANES), F32)
    tokens = call(
        lambda *r: pack_kernel(plan, *r),
        message,
        (state[0], norm_gains, channel_biases, up_bias.reshape(1, ch * wide)),
        [pltpu.VMEM((plan.tokens, wide), F32)]
        + [pltpu.VMEM((rows, width, LANES), F32)] * 2
        + [pltpu.VMEM(v.shape, BF) for v in (norm_gains, channel_biases, up_bias.reshape(1, -1))]
        + [pltpu.SemaphoreType.DMA((3,))],
        10**8,
        far_in=3,
        grant=PACK,
    )
    got = exchange(tokens, "ch")

    half, own = up_weight.shape[1] // 2, down_weight.shape[0] // PART
    shapes = [(D, half), (own, D), (down_weight.shape[0] - 2 * own, D)]
    parts = [jax.ShapeDtypeStruct(shape, BF) for shape in shapes]
    up_part, own_part, rest_part = call(
        parts_kernel,
        tuple(parts),
        (up_weight, down_weight),
        [pltpu.VMEM(t.shape, BF) for t in parts] + [pltpu.SemaphoreType.DMA((6,))],
        10**6,
        far_in=2,
        far_out=(0, 1, 2),
        grant=58,
    )
    up_a = across(up_part, far)
    span = LANES * high_units(plan)
    blocks = [jax.ShapeDtypeStruct((filter_in.shape[1], span, span), BF)] * 4
    blocks += [jax.ShapeDtypeStruct((1, 2 * wide), F32)] * 2
    blocks = call(
        lambda *r: block_kernel(plan, *r),
        tuple(blocks),
        (filter_in, filter_in_bias, filter_out, filter_out_bias),
        [pltpu.VMEM(t.shape, t.dtype) for t in blocks] + [pltpu.SemaphoreType.DMA((6,))],
        10**8,
        far_out=range(6),
        grant=58,
    )
    got, *blocks = lax.optimization_barrier((got, *blocks))
    up_c, down_c = across(up_weight, 1), across(down_weight, 1)

    short = jnp.asarray(short_tables(plan))
    odd = np.tile(np.repeat(np.arange(plan.slots) % 2, plan.height), plan.per)
    sign = np.where((odd[:, None] == 1) & (np.arange(LANES)[None] >= HALF), -1.0, 1.0)
    sign = sign.astype(np.float32)

    wire = jax.ShapeDtypeStruct((plan.peers, plan.message, LANES), BF)
    held = jax.ShapeDtypeStruct((plan.tokens, D), F32)
    scratch = [pltpu.VMEM((plan.lat, ch, plan.message, LANES), F32)]
    begun = jax.ShapeDtypeStruct((plan.tokens + 16 + short.shape[1], D), F32)
    assert short.shape[1] <= D - 256
    begun, sent = call(
        lambda *r: start_kernel(plan, *r),
        (begun, wire),
        (got, short),
        scratch
        + [pltpu.VMEM(t.shape, t.dtype) for t in (short, begun)]
        + [pltpu.SemaphoreType.DMA((2,))],
        10**9,
        far_in=1,
        far_out=(0,),
        grant=START,
    )
    row, col = mode_places(plan)
    lines = plan.peers * (plan.main + plan.left)
    dims = [(plan.modes, 2 * lines)] * 2 + [(lines, 2 * plan.modes)] * 2
    tables = [jax.ShapeDtypeStruct(shape, BF) for shape in dims]
    for step_index in range(STEPS):
        first, last = step_index == 0, step_index == STEPS - 1
        arrived = exchange(sent, both)
        if first:
            down_a = across(own_part, far)
            rest = across(rest_part, far)
            up_b = beside(up_a)
            up_ac = across(up_a, 1)
        if first:
            sent, *tables = call(
                lambda *r: spectral_kernel(plan, True, *r),
                (wire, *tables),
                (arrived, row.T, col, row, col.T, sign, *blocks),
                [pltpu.VMEM((plan.peers, plan.message, LANES), F32)]
                + [pltpu.SemaphoreType.DMA((10,))]
                + [pltpu.VMEM(t.shape, t.dtype) for t in (*tables, *blocks)],
                10**9,
                far_in=6,
                far_out=range(1, 5),
                grant=FIRST,
            )
        else:
            sent = call(
                lambda *r: spectral_kernel(plan, False, *r),
                wire,
                (arrived, *tables, *blocks, sign),
                [pltpu.VMEM((plan.peers, plan.message, LANES), F32)],
                10**9,
            )
        if first:
            up_bc = across(after(up_b, sent), 1)
            down_b = beside(after(down_a, sent))
            down_ac = across(after(down_a, sent), 1)
            down_bc = across(after(down_b, sent), 1)
            rest_c = across(after(rest, sent), 1)
        arrived = exchange(sent, both)
        if first:
            near = (up_weight, down_weight, up_c, down_c)
            distant = (up_a, up_b, down_a, down_b, rest, up_ac, up_bc, down_ac, down_bc, rest_c)
            sources = (begun, *near, *distant)
            total, sent, params, ups, downs = call(
                lambda *r: token_kernel(plan, True, False, *r),
                (
                    held,
                    wire,
                    jax.ShapeDtypeStruct((16, D), F32),
                    jax.ShapeDtypeStruct((D, ch * up_weight.shape[1]), BF),
                    jax.ShapeDtypeStruct((ch * down_weight.shape[0], D), BF),
                ),
                (arrived, *sources),
                scratch
                + [pltpu.SemaphoreType.DMA((len(sources),))]
                + [pltpu.VMEM(t.shape, t.dtype) for t in (begun, short)],
                10**10,
                        far_in=len(sources),
                grant=24,
            )
            continue
        result = call(
            lambda *r: token_kernel(plan, False, last, *r),
            message if last else (held, wire),
            (arrived, total, short, params, ups, downs),
            scratch,
            10**10,
        )
        if not last:
            total, sent = result
    result = exchange(result, "ch")
    result = call(
        lambda *r: unpack_kernel(plan, *r),
        jax.ShapeDtypeStruct((rows, width, wide), F32),
        (result,),
        [pltpu.VMEM((rows, width, LANES), F32)] * 2,
        10**8,
    )
    return result[None]


def solution(mesh):
    placed = (
        P(None, "lat", None, "ch"),
        P(None, "ch"),
        P(None, "ch"),
        P(None, "ch", None, None),
        P(None, "ch", None),
        P(None, "ch", None, None),
        P(None, "ch", None),
        P(None, "ch"),
        P("ch"),
        P("ch", None),
    )

    return jax.shard_map(
        local, mesh=mesh, in_specs=placed, out_specs=P(None, "lat", None, "ch"), check_vma=False
    )
```

```python
import math

import jax
import jax.numpy as jnp
import numpy as np
from jax import lax
from jax.experimental import pallas as pl
from jax.experimental.pallas import tpu as pltpu
from jax.sharding import PartitionSpec as P


D = 768
M = 64
STEPS = 4
EPS = 1e-05
SHRINK = 0.01
HALF = 64
PACK, START, FIRST = 24, 24, 58
PART = 4
LANES = 128
BF = jnp.bfloat16
F32 = jnp.float32


class Plan:
    def __init__(self, lat, ch, rows, width):
        self.lat, self.ch, self.rows, self.width = lat, ch, rows, width
        self.height = rows * lat
        self.short = width // ch
        self.padded = -(-self.short // 16) * 16
        self.tokens = rows * self.padded
        self.classes = self.short // 2 + 1
        self.per = -(-self.classes // lat)
        self.wide = D // ch
        self.units = self.wide // HALF
        self.items = rows * self.per
        spare = self.items % 8
        if self.items > 8 and spare and spare * self.units <= 8:
            self.main, self.left = self.items - spare, spare
        else:
            self.main, self.left = -(-self.items // 8) * 8, 0
        self.message = self.units * self.main + (8 if self.left else 0)
        slots = 0
        while (slots // 2) * self.short + (slots % 2) * (self.short - self.short // 2) < M:
            slots += 1
        self.slots = slots
        self.modes = self.per * slots * self.height
        self.peers = lat * ch
        self.spare = self.padded - self.short
        self.packed = self.tokens + self.tokens // 2
        hj = np.arange(self.main)
        self.item_h = np.where(hj < self.items, hj // self.per, 0)
        self.item_j = np.where(hj < self.items, hj % self.per, -1)
        tail = self.main + np.arange(self.left)
        self.tail_h, self.tail_j = tail // self.per, tail % self.per


def split_np(table):
    hi = table.astype(np.float32).astype(BF)
    lo = (table - hi.astype(np.float64)).astype(np.float32).astype(BF)
    return hi, lo


def short_tables(plan):
    g = np.arange(plan.lat)
    item_g = np.concatenate([np.repeat(g, plan.main), np.repeat(g, plan.left)])
    item_h = np.concatenate([np.tile(plan.item_h, plan.lat), np.tile(plan.tail_h, plan.lat)])
    item_j = np.concatenate([np.tile(plan.item_j, plan.lat), np.tile(plan.tail_j, plan.lat)])
    order = item_g * plan.per + item_j
    good = (item_j >= 0) & (order < plan.classes)
    tok_h = np.repeat(np.arange(plan.rows), plan.padded)
    tok_a = np.tile(np.arange(plan.padded), plan.rows)
    mask = good[:, None] & (item_h[:, None] == tok_h[None]) & (tok_a[None] < plan.short)
    angle = 2 * np.pi / plan.short * (order[:, None] * tok_a[None] % plan.short)
    cos, sin = np.cos(angle) * mask, np.sin(angle) * mask
    forward = np.concatenate([cos, -sin], 0)
    inverse = np.concatenate([cos.T, -sin.T], 1)
    side = max(forward.shape)
    tables = [np.pad(t, [(0, side - n) for n in t.shape]) for t in (forward, inverse)]
    return np.stack(split_np(tables[0]) + split_np(tables[1]))


def mode_places(plan):
    j, t, k = (
        v.reshape(-1)
        for v in np.meshgrid(
            np.arange(plan.per), np.arange(plan.slots), np.arange(plan.height), indexing="ij"
        )
    )
    peer = np.arange(plan.peers)
    col_p = np.concatenate([np.repeat(peer, plan.main), np.repeat(peer, plan.left)])
    col_h = np.concatenate([np.tile(plan.item_h, plan.peers), np.tile(plan.tail_h, plan.peers)])
    col_j = np.concatenate([np.tile(plan.item_j, plan.peers), np.tile(plan.tail_j, plan.peers)])
    col_h = (col_p // plan.ch) * plan.rows + col_h
    none = np.zeros_like(j)
    row = np.stack([j, t % 2, (t + 1) // 2, k] + [none] * 4).astype(np.float32)
    none = np.zeros_like(col_p)
    col = np.stack([col_p % plan.ch, col_h, col_j] + [none] * 5).astype(np.float32)
    return row, col


def cos_sin(turns):
    turns = turns - jnp.floor(turns + 0.5)
    quarter = jnp.floor(turns * 4.0 + 0.5)
    x = (turns - quarter * 0.25) * (2.0 * math.pi)
    y = x * x
    sin = x * (1 + y * (-1 / 6 + y * (1 / 120 + y * (-1 / 5040 + y * (1 / 362880)))))
    cos = 1 + y * (-0.5 + y * (1 / 24 + y * (-1 / 720 + y * (1 / 40320 - y * (1 / 3628800)))))
    odd = jnp.abs(quarter) == 1.0
    c, s = jnp.where(odd, sin, cos), jnp.where(odd, cos, sin)
    c = jnp.where((quarter == 1.0) | (jnp.abs(quarter) == 2.0), -c, c)
    s = jnp.where((quarter == -1.0) | (jnp.abs(quarter) == 2.0), -s, s)
    return c, s


def mode_table(plan, first_class, row, col):
    j, odd, times, k = row
    q, h, col_j = col
    order = first_class + j
    mode = times * plan.short + jnp.where(odd == 1.0, -order, order)
    fine = (mode < M) & (order < plan.classes)
    fine = fine & ((order > 0.0) | (times == 0.0) | (odd == 1.0))
    fine = fine & ((2.0 * order != plan.short) | (odd == 0.0))
    scale = 1.0 / math.sqrt(plan.height * plan.width)
    weight = jnp.where(fine, scale, 0.0)
    doubled = jnp.where(mode == 0.0, 1.0, 2.0)
    turn = jnp.where(odd == 1.0, 1.0, -1.0)
    product = k * h
    product = product - plan.height * jnp.floor(product * (1.0 / plan.height) + 1e-4)
    cos, sin = cos_sin(mode * q * (1.0 / plan.width) + product * (1.0 / plan.height))
    keep = jnp.where(j == col_j, weight, 0.0)
    return cos * keep, sin * (keep * turn), doubled


def split(value):
    hi = value.astype(BF)
    return hi, (value - hi.astype(F32)).astype(BF)


def dot(a, b):
    return jnp.dot(a, b, preferred_element_type=F32)


def low_lanes(shape):
    return lax.broadcasted_iota(jnp.int32, shape, len(shape) - 1) % LANES < HALF


def swap(value):
    return pltpu.roll(value, HALF, 1)


def norm(values, gain, shift):
    mean = jnp.sum(values, -1, keepdims=True) * (1.0 / D)
    spread = jnp.sum(values * values, -1, keepdims=True) * (1.0 / D) - mean * mean
    return (values - mean) * lax.rsqrt(spread + EPS) * gain + shift


def emit_wire(plan, normed, tab, wire_ref, scratch):
    hi, lo = split(normed)
    count = plan.lat * plan.main
    half = count + plan.lat * plan.left
    fhi, flo = tab[0, : 2 * half, : plan.tokens], tab[1, : 2 * half, : plan.tokens]
    spec = dot(fhi, hi) + dot(flo, hi) + dot(fhi, lo)
    low = low_lanes((half, LANES))
    for tile in range(D // LANES):
        lanes = slice(tile * LANES, (tile + 1) * LANES)
        re, im = spec[:half, lanes], spec[half:, lanes]
        pair = (jnp.where(low, re, swap(im)), jnp.where(low, swap(re), im))
        for which in range(2):
            c, u = divmod(2 * tile + which, plan.units)
            part = pair[which]
            scratch[:, c, u * plan.main : (u + 1) * plan.main, :] = part[:count].reshape(
                plan.lat, plan.main, LANES
            )
            for spot in range(plan.left):
                row = plan.units * plan.main + u * plan.left + spot
                for g in range(plan.lat):
                    at = count + g * plan.left + spot
                    scratch[g, c, row : row + 1, :] = part[at : at + 1]
    if plan.left:
        first = plan.units * (plan.main + plan.left)
        if first < plan.message:
            scratch[:, :, first:, :] = jnp.zeros(
                (plan.lat, plan.ch, plan.message - first, LANES), F32
            )
    wire_ref[...] = scratch[...].reshape(plan.peers, plan.message, LANES).astype(BF)


def read_wire(plan, wire_ref, tab, scratch):
    scratch[...] = wire_ref[...].astype(F32).reshape(plan.lat, plan.ch, plan.message, LANES)
    count = plan.lat * plan.main
    half = count + plan.lat * plan.left
    low = low_lanes((half, LANES))

    def unit(index):
        c, u = divmod(index, plan.units)
        parts = [scratch[:, c, u * plan.main : (u + 1) * plan.main, :].reshape(count, LANES)]
        for g in range(plan.lat):
            for spot in range(plan.left):
                row = plan.units * plan.main + u * plan.left + spot
                parts.append(scratch[g, c, row : row + 1, :])
        return jnp.concatenate(parts, 0) if len(parts) > 1 else parts[0]

    tiles = []
    for tile in range(D // LANES):
        a, b = unit(2 * tile), unit(2 * tile + 1)
        re = jnp.where(low, a, swap(b))
        im = jnp.where(low, swap(a), b)
        tiles.append(jnp.concatenate([re, im], 0).astype(BF))
    right = jnp.concatenate(tiles, 1)
    ghi, glo = tab[2, : plan.tokens, : 2 * half], tab[3, : plan.tokens, : 2 * half]
    return dot(ghi, right) + dot(glo, right)


def pack(values):
    half = values.shape[0] // 2
    tail = values[:, LANES:]
    return jnp.concatenate([values[:, :LANES], jnp.concatenate([tail[:half], tail[half:]], 1)], 0)


def unpack(message):
    tokens = message.shape[0] // 3 * 2
    tail = message[tokens:]
    tail = jnp.concatenate([tail[:, :HALF], tail[:, HALF:]], 0)
    return jnp.concatenate([message[:tokens], tail], 1)


def pack_kernel(plan, state_ref, gain_hbm, bias_hbm, up_hbm, *refs):
    outs, (scratch, body, tail, out_ref, gain_ref, bias_ref, up_ref, sem) = refs[: plan.ch], refs[plan.ch :]
    copies = fetch([gain_hbm, bias_hbm, up_hbm], [gain_ref, bias_ref, up_ref], sem)
    body[...] = state_ref[:, :, :LANES]
    tail[:, :, :HALF] = state_ref[:, :, LANES:]
    for copy in copies:
        copy.wait()
    line = up_ref[...].astype(F32)
    small = [gain_ref[...].astype(F32), bias_ref[...].astype(F32)]
    small += [line[:, n * plan.wide : (n + 1) * plan.wide] for n in range(plan.ch)]
    small = jnp.concatenate(small, 0)
    count = small.shape[0]
    scratch[...] = jnp.zeros(scratch.shape, F32)
    for n in range(count):
        h, s = divmod(n, plan.spare)
        at = h * plan.padded + plan.short + s
        scratch[at : at + 1, :] = small[n : n + 1]
    for q in range(plan.ch):
        for h in range(plan.rows):
            at = h * plan.padded
            every = pl.ds(q, plan.short, stride=plan.ch)
            scratch[at : at + plan.short, :LANES] = body[h, every, :]
            scratch[at : at + plan.short, LANES:] = tail[h, every, :][:, :HALF]
        out_ref[q] = pack(scratch[...])
    for n in range(plan.ch):
        outs[n][...] = out_ref[lax.axis_index("ch") ^ n]


def unpack_kernel(plan, *refs):
    got, (out_ref, body, tail) = refs[: plan.ch], refs[plan.ch :]
    for n in range(plan.ch):
        q = lax.axis_index("ch") ^ n
        values = unpack(got[n][...])
        wide = jnp.concatenate([values[:, LANES:], values[:, LANES:]], 1)
        for h in range(plan.rows):
            at = slice(h * plan.padded, h * plan.padded + plan.short)
            every = pl.ds(q, plan.short, stride=plan.ch)
            body[h, every, :] = values[at, :LANES]
            tail[h, every, :] = wide[at]
    out_ref[:, :, :LANES] = body[...]
    out_ref[:, :, LANES:] = tail[:, :, :HALF]


def fetch(sources, targets, sem):
    copies = [pltpu.make_async_copy(a, b, sem.at[n]) for n, (a, b) in enumerate(zip(sources, targets))]
    for copy in copies:
        copy.start()
    return copies


def parts_kernel(up_ref, down_ref, up_out, own_out, rest_out, *refs):
    mids, sem = refs[:3], refs[3]
    half, own = up_out.shape[1], own_out.shape[0]
    side = lax.axis_index("lat") % 2
    at = pl.multiple_of(side * half, LANES)
    to = pl.multiple_of(side * own, HALF)
    into = fetch(
        [up_ref.at[:, pl.ds(at, half)], down_ref.at[pl.ds(to, own), :], down_ref.at[2 * own :, :]],
        mids,
        sem,
    )
    away = []
    for n, out in enumerate((up_out, own_out, rest_out)):
        into[n].wait()
        away.append(pltpu.make_async_copy(mids[n], out, sem.at[3 + n]))
        away[n].start()
    for copy in away:
        copy.wait()


def fill_tables(plan, rowv, colv, rowt, colt, chi, clo, ehi, elo):
    first = (lax.axis_index("lat") * plan.per).astype(F32)
    size = plan.modes
    wide = plan.peers * (plan.main + plan.left)
    rows = [rowv[:, n : n + 1] for n in range(4)]
    cols = [colv[n : n + 1, :] for n in range(3)]
    cos, sin, _ = mode_table(plan, first, rows, cols)
    chi[:, :wide], clo[:, :wide] = split(cos)
    chi[:, wide:], clo[:, wide:] = split(sin)
    rows = [rowt[n : n + 1, :] for n in range(4)]
    cols = [colt[:, n : n + 1] for n in range(3)]
    cos, sin, doubled = mode_table(plan, first, rows, cols)
    ehi[:, :size], elo[:, :size] = split(cos * doubled)
    ehi[:, size:], elo[:, size:] = split(-sin * doubled)


def high_units(plan):
    return plan.units - 1


def block_kernel(plan, fin, finb, fout, foutb, *refs):
    outs, (w1h, w1l, w2h, w2l, b1, b2), sem = refs[:6], refs[6:12], refs[12]
    copies = [pltpu.make_async_copy(a, b, sem.at[n]) for n, (a, b) in enumerate(zip(refs[6:12], outs))]
    span = high_units(plan)
    for weights, bias, high, low, out in ((fin, finb, w1h, w1l, b1), (fout, foutb, w2h, w2l, b2)):
        blocks, channels = weights.shape[1], weights.shape[2]
        for n in range(blocks):
            full = []
            for p in range(2):
                lines = [jnp.zeros((channels, blocks * channels), F32)] * blocks
                cells = [jnp.zeros((channels, channels), F32)] * blocks
                cells[n] = weights[p, n]
                lines[n] = jnp.concatenate(cells, 1)
                full.append(jnp.concatenate(lines, 0))
            for u in range(n, n + span):
                at = slice(u * HALF, (u + 1) * HALF)
                real, imag = full[0][at], full[1][at]
                for p, (left, right) in enumerate(((real, imag), (-imag, real))):
                    cells = []
                    for v in range(n, n + span):
                        cut = slice(v * HALF, (v + 1) * HALF)
                        cells += [left[:, cut], right[:, cut]]
                    row = jnp.concatenate(cells, 1)
                    to = slice((2 * (u - n) + p) * HALF, (2 * (u - n) + p + 1) * HALF)
                    high[n, to, :], low[n, to, :] = split(row)
        lines = [jnp.concatenate([bias[p, n : n + 1] for n in range(blocks)], 1) for p in range(2)]
        cells = []
        for v in range(plan.units):
            cells += [line[:, v * HALF : (v + 1) * HALF] for line in lines]
        out[...] = jnp.concatenate(cells, 1)
    for copy in copies:
        copy.start()
    for copy in copies:
        copy.wait()


def start_kernel(plan, *refs):
    came, (tab_hbm, begun_hbm, wire_ref, scratch, got_ref, tab, begun, sem) = refs[: plan.ch], refs[plan.ch :]
    for n in range(plan.ch):
        got_ref[lax.axis_index("ch") ^ n] = came[n][...]
    sum_ref, par_ref = begun.at[: plan.tokens], begun.at[plan.tokens : plan.tokens + 16]
    bias_ref = par_ref.at[8:16]
    copies = fetch([tab_hbm], [tab], sem)
    got = [unpack(got_ref[c]) for c in range(plan.ch)]
    full = jnp.concatenate(got, 1)
    rows = []
    for h in range(plan.rows):
        for s in range(plan.spare):
            rows.append(h * plan.padded + plan.short + s)
    for n in range(5):
        par_ref[n : n + 1, :] = full[rows[n] : rows[n] + 1, :]
    par_ref[5:8, :] = jnp.zeros((3, D), F32)
    bias_ref[...] = jnp.zeros(bias_ref.shape, F32)
    for s in range(plan.ch):
        source = unpack(came[s][...])
        parts = [source[rows[5 + n] : rows[5 + n] + 1, :] for n in range(plan.ch)]
        line = jnp.concatenate(parts, 1)
        bias_ref[s : s + 1, :] = line
    inside = lax.broadcasted_iota(jnp.int32, (plan.tokens, 1), 0) % plan.padded < plan.short
    values = jnp.where(inside, full, 0.0)
    normed = norm(values, par_ref[0:1, :], par_ref[2:3, :])
    sum_ref[...] = values + normed
    copies[0].wait()
    side = tab.shape[1]
    rows = slice(plan.tokens + 16, plan.tokens + 16 + side)
    for n in range(2):
        whole = tab[2 * n].astype(F32) + tab[2 * n + 1].astype(F32)
        begun[rows, 256 * n : 256 * n + side] = whole
    copies.append(pltpu.make_async_copy(begun, begun_hbm, sem.at[1]))
    copies[1].start()
    emit_wire(plan, normed, tab, wire_ref, scratch)
    copies[1].wait()


def token_kernel(plan, first, last, *refs):
    copies = []
    if first:
        wire_in, sources, refs = refs[0], refs[1:16], refs[16:]
        (sum_out, wire_out, par_out, up_all, down_all), refs = refs[:5], refs[5:]
        scratch, sem, (begun, tab) = refs[0], refs[1], refs[2:]
        sum_in, par_ref = begun.at[: plan.tokens], begun.at[plan.tokens : plan.tokens + 16]
        shard = up_all.shape[1] // plan.ch
        half, own = shard // 2, shard // PART
        y = lax.axis_index("lat") % 2
        copies = fetch(sources[:1], (begun,), sem)
        groups = []
        weights = sources[1:]
        for s in range(plan.ch):
            at = s * shard
            if s < plan.ch // 2:
                ups, downs = weights[:1], weights[1:2]
                weights = weights[2:]
                ups = [(ups[0], up_all.at[:, at : at + shard])]
                downs = [(downs[0], down_all.at[at : at + shard, :])]
            else:
                ups, downs = weights[:2], weights[2:5]
                spots = [pl.multiple_of(at + n * half, LANES) for n in (y, 1 - y)]
                ups = [(w, up_all.at[:, pl.ds(n, half)]) for w, n in zip(ups, spots)]
                spots = [pl.multiple_of(at + n * own, HALF) for n in (y, 1 - y)]
                spots.append(at + 2 * own)
                sizes = (own, own, shard - 2 * own)
                downs = [
                    (w, down_all.at[pl.ds(n, size), :]) for w, n, size in zip(downs, spots, sizes)
                ]
                weights = weights[5:]
            group = []
            for source, target in ups + downs:
                count = len(copies)
                copies.append(pltpu.make_async_copy(source, target, sem.at[count]))
                copies[-1].start()
                group.append(copies[-1])
            groups.append(group)
        copies[0].wait()
        side = tab.shape[1]
        for n in range(2):
            whole = begun[plan.tokens + 16 :, 256 * n : 256 * n + side]
            tab[2 * n], tab[2 * n + 1] = split(whole)
        par_out[...] = par_ref[...]
    else:
        wire_in, sum_in, tab, par_ref, up_all, down_all = refs[:6]
        outs, scratch = refs[6:], refs[-1]
        if last:
            outs, scratch = refs[6:], refs[-2]
        shard = up_all.shape[1] // plan.ch
        half = shard // 2
    values = sum_in[...] + read_wire(plan, wire_in, tab, scratch)
    normed = norm(values, par_ref[1:2, :], par_ref[3:4, :]).astype(BF)
    mixed = par_ref[4:5, :]
    for s in range(2 * plan.ch):
        if first and s % 2 == 0:
            for copy in groups[s // 2]:
                copy.wait()
        at = slice((s % 2) * half, (s % 2 + 1) * half)
        cut = slice(s * half, (s + 1) * half)
        bias = par_ref[8 + s // 2 : 9 + s // 2, at]
        pre = dot(normed, up_all[:, cut]) + bias
        hidden = (0.5 * pre * (1.0 + lax.erf(pre * math.sqrt(0.5)))).astype(BF)
        mixed = mixed + dot(hidden, down_all[cut, :])
    values = values + mixed
    if last:
        for c in range(plan.ch):
            refs[-1][c] = pack(values[:, c * plan.wide : (c + 1) * plan.wide])
        for n in range(plan.ch):
            outs[n][...] = refs[-1][lax.axis_index("ch") ^ n]
        return
    if not first:
        sum_out, wire_out = outs[:2]
    normed = norm(values, par_ref[0:1, :], par_ref[2:3, :])
    sum_out[...] = values + normed
    emit_wire(plan, normed, tab, wire_out, scratch)


def spectral_kernel(plan, far, wire_in, *refs):
    copies, away = [], []
    if far:
        places, sign_ref, sources, wire_out = refs[:4], refs[4], refs[5:11], refs[11]
        outs, scratch, sem = refs[12:16], refs[16], refs[17]
        chi, clo, ehi, elo = tables = refs[18:22]
        w1h, w1l, w2h, w2l, b1, b2 = mids = refs[22:]
        copies = fetch(sources, mids, sem)
        fill_tables(plan, *places, *tables)
        for n, (table, out) in enumerate(zip(tables, outs)):
            away.append(pltpu.make_async_copy(table, out, sem.at[6 + n]))
            away[n].start()
    else:
        chi, clo, ehi, elo, w1h, w1l, w2h, w2l, b1, b2, sign_ref, wire_out, scratch = refs
    scratch[...] = wire_in[...].astype(F32)
    count = plan.peers * plan.main
    half = count + plan.peers * plan.left
    low = low_lanes((half, LANES))
    pieces = []
    for u in range(plan.units):
        parts = [scratch[:, u * plan.main : (u + 1) * plan.main, :].reshape(count, LANES)]
        for p in range(plan.peers if plan.left else 0):
            row = plan.units * plan.main + u * plan.left
            parts.append(scratch[p, row : row + plan.left, :])
        data = jnp.concatenate(parts, 0) if len(parts) > 1 else parts[0]
        turned = swap(data)
        turned = jnp.where(low, -turned, turned)
        pieces.append(jnp.concatenate([data, turned], 0).astype(BF))
    right = jnp.concatenate(pieces, 1)

    def ready(*which):
        for n in which if far else ():
            copies[n].wait()

    spec = dot(chi[...], right) + dot(clo[...], right)
    sign = jnp.concatenate([sign_ref[...]] * plan.units, 1)
    spec = spec * sign

    def layer(value, wh, wl, bias):
        hi, lo = split(value)
        span, total = wh.shape[1], 0.0
        for n in range(wh.shape[0]):
            cut = slice(n * LANES, n * LANES + span)
            part = dot(hi[:, cut], wh[n]) + dot(hi[:, cut], wl[n]) + dot(lo[:, cut], wh[n])
            sides = [(part.shape[0], n * LANES), (part.shape[0], value.shape[1] - span - n * LANES)]
            cells = [jnp.zeros(sides[0], F32)] * (n > 0) + [part]
            cells += [jnp.zeros(sides[1], F32)] * (sides[1][1] > 0)
            total = total + jnp.concatenate(cells, 1)
        return total + bias[...]

    ready(0, 1, 4)
    first = jnp.maximum(layer(spec, w1h, w1l, b1), 0.0)
    ready(2, 3, 5)
    second = layer(first, w2h, w2l, b2)
    shrunk = jnp.where(
        second > SHRINK, second - SHRINK, jnp.where(second < -SHRINK, second + SHRINK, 0.0)
    )
    shrunk = shrunk * sign
    low = low_lanes((plan.modes, LANES))
    pieces = []
    for u in range(plan.units):
        part = shrunk[:, u * LANES : (u + 1) * LANES]
        turned = swap(part)
        pieces.append(jnp.concatenate([part, jnp.where(low, -turned, turned)], 0))
    hi, lo = split(jnp.concatenate(pieces, 1))
    back = dot(ehi[...], hi) + dot(elo[...], hi) + dot(ehi[...], lo)
    for u in range(plan.units):
        part = back[:, u * LANES : (u + 1) * LANES]
        scratch[:, u * plan.main : (u + 1) * plan.main, :] = part[:count].reshape(
            plan.peers, plan.main, LANES
        )
        row = plan.units * plan.main + u * plan.left
        for p in range(plan.peers if plan.left else 0):
            at = count + p * plan.left
            scratch[p, row : row + plan.left, :] = part[at : at + plan.left]
    wire_out[...] = scratch[...].astype(BF)
    for copy in away:
        copy.wait()


def call(body, outs, operands, scratch, flops, far_in=0, far_out=(), grant=20):
    vmem = pl.BlockSpec(memory_space=pltpu.VMEM)
    anywhere = pl.BlockSpec(memory_space=pl.ANY)
    flat, tree = jax.tree.flatten(outs)
    out_specs = [anywhere if n in far_out else vmem for n in range(len(flat))]
    return pl.pallas_call(
        body,
        out_shape=outs,
        in_specs=[vmem] * (len(operands) - far_in) + [anywhere] * far_in,
        out_specs=jax.tree.unflatten(tree, out_specs),
        scratch_shapes=scratch,
        compiler_params=pltpu.CompilerParams(vmem_limit_bytes=grant * 2**20),
        cost_estimate=pl.CostEstimate(flops=flops, bytes_accessed=2**20, transcendentals=0),
    )(*operands)


def local(
    state,
    norm_gains,
    channel_biases,
    filter_in,
    filter_in_bias,
    filter_out,
    filter_out_bias,
    up_weight,
    up_bias,
    down_weight,
):
    _, rows, width, wide = state.shape
    plan = Plan(lax.axis_size("lat"), lax.axis_size("ch"), rows, width)
    ch = plan.ch
    far = ch // 2
    both = ("lat", "ch")
    assert plan.spare * rows >= 5 + ch and up_bias.shape[0] == ch * wide

    def across(value, step):
        return lax.ppermute(value, "ch", [(i, i ^ step) for i in range(ch)])

    def beside(value):
        return lax.ppermute(value, "lat", [(i, i ^ 1) for i in range(plan.lat)])

    def exchange(value, axes):
        return lax.all_to_all(value, axes, 0, 0, tiled=True)

    def after(value, token):
        return lax.optimization_barrier((value, token))[0]

    message = (jax.ShapeDtypeStruct((plan.packed, LANES), F32),) * ch
    mail = pltpu.VMEM((ch, plan.packed, LANES), F32)
    tokens = call(
        lambda *r: pack_kernel(plan, *r),
        message,
        (state[0], norm_gains, channel_biases, up_bias.reshape(1, ch * wide)),
        [pltpu.VMEM((plan.tokens, wide), F32)]
        + [pltpu.VMEM((rows, width, LANES), F32)] * 2
        + [mail]
        + [pltpu.VMEM(v.shape, BF) for v in (norm_gains, channel_biases, up_bias.reshape(1, -1))]
        + [pltpu.SemaphoreType.DMA((3,))],
        10**8,
        far_in=3,
        grant=PACK,
    )
    got = [tokens[0]] + [across(tokens[n], n) for n in range(1, ch)]

    half, own = up_weight.shape[1] // 2, down_weight.shape[0] // PART
    shapes = [(D, half), (own, D), (down_weight.shape[0] - 2 * own, D)]
    parts = [jax.ShapeDtypeStruct(shape, BF) for shape in shapes]
    up_part, own_part, rest_part = call(
        parts_kernel,
        tuple(parts),
        (up_weight, down_weight),
        [pltpu.VMEM(t.shape, BF) for t in parts] + [pltpu.SemaphoreType.DMA((6,))],
        10**6,
        far_in=2,
        far_out=(0, 1, 2),
        grant=58,
    )
    up_a = across(up_part, far)
    span = LANES * high_units(plan)
    blocks = [jax.ShapeDtypeStruct((filter_in.shape[1], span, span), BF)] * 4
    blocks += [jax.ShapeDtypeStruct((1, 2 * wide), F32)] * 2
    blocks = call(
        lambda *r: block_kernel(plan, *r),
        tuple(blocks),
        (filter_in, filter_in_bias, filter_out, filter_out_bias),
        [pltpu.VMEM(t.shape, t.dtype) for t in blocks] + [pltpu.SemaphoreType.DMA((6,))],
        10**8,
        far_out=range(6),
        grant=58,
    )
    got[1], *blocks = lax.optimization_barrier((got[1], *blocks))
    up_c, down_c = across(up_weight, 1), across(down_weight, 1)

    short = jnp.asarray(short_tables(plan))
    odd = np.tile(np.repeat(np.arange(plan.slots) % 2, plan.height), plan.per)
    sign = np.where((odd[:, None] == 1) & (np.arange(LANES)[None] >= HALF), -1.0, 1.0)
    sign = sign.astype(np.float32)

    wire = jax.ShapeDtypeStruct((plan.peers, plan.message, LANES), BF)
    held = jax.ShapeDtypeStruct((plan.tokens, D), F32)
    scratch = [pltpu.VMEM((plan.lat, ch, plan.message, LANES), F32)]
    begun = jax.ShapeDtypeStruct((plan.tokens + 16 + short.shape[1], D), F32)
    assert short.shape[1] <= D - 256
    begun, sent = call(
        lambda *r: start_kernel(plan, *r),
        (begun, wire),
        (*got, short),
        scratch
        + [mail]
        + [pltpu.VMEM(t.shape, t.dtype) for t in (short, begun)]
        + [pltpu.SemaphoreType.DMA((2,))],
        10**9,
        far_in=1,
        far_out=(0,),
        grant=START,
    )
    row, col = mode_places(plan)
    lines = plan.peers * (plan.main + plan.left)
    dims = [(plan.modes, 2 * lines)] * 2 + [(lines, 2 * plan.modes)] * 2
    tables = [jax.ShapeDtypeStruct(shape, BF) for shape in dims]
    for step_index in range(STEPS):
        first, last = step_index == 0, step_index == STEPS - 1
        arrived = exchange(sent, both)
        if first:
            down_a = across(own_part, far)
            rest = across(rest_part, far)
            up_b = beside(up_a)
            up_ac = across(up_a, 1)
        if first:
            sent, *tables = call(
                lambda *r: spectral_kernel(plan, True, *r),
                (wire, *tables),
                (arrived, row.T, col, row, col.T, sign, *blocks),
                [pltpu.VMEM((plan.peers, plan.message, LANES), F32)]
                + [pltpu.SemaphoreType.DMA((10,))]
                + [pltpu.VMEM(t.shape, t.dtype) for t in (*tables, *blocks)],
                10**9,
                far_in=6,
                far_out=range(1, 5),
                grant=FIRST,
            )
        else:
            sent = call(
                lambda *r: spectral_kernel(plan, False, *r),
                wire,
                (arrived, *tables, *blocks, sign),
                [pltpu.VMEM((plan.peers, plan.message, LANES), F32)],
                10**9,
            )
        if first:
            up_bc = across(after(up_b, sent), 1)
            down_b = beside(after(down_a, sent))
            down_ac = across(after(down_a, sent), 1)
            down_bc = across(after(down_b, sent), 1)
            rest_c = across(after(rest, sent), 1)
        arrived = exchange(sent, both)
        if first:
            near = (up_weight, down_weight, up_c, down_c)
            distant = (up_a, up_b, down_a, down_b, rest, up_ac, up_bc, down_ac, down_bc, rest_c)
            sources = (begun, *near, *distant)
            total, sent, params, ups, downs = call(
                lambda *r: token_kernel(plan, True, False, *r),
                (
                    held,
                    wire,
                    jax.ShapeDtypeStruct((16, D), F32),
                    jax.ShapeDtypeStruct((D, ch * up_weight.shape[1]), BF),
                    jax.ShapeDtypeStruct((ch * down_weight.shape[0], D), BF),
                ),
                (arrived, *sources),
                scratch
                + [pltpu.SemaphoreType.DMA((len(sources),))]
                + [pltpu.VMEM(t.shape, t.dtype) for t in (begun, short)],
                10**10,
                        far_in=len(sources),
                grant=24,
            )
            continue
        result = call(
            lambda *r: token_kernel(plan, False, last, *r),
            message if last else (held, wire),
            (arrived, total, short, params, ups, downs),
            scratch + [mail] * last,
            10**10,
        )
        if not last:
            total, sent = result
    result = [result[0]] + [across(result[n], n) for n in range(1, ch)]
    result = call(
        lambda *r: unpack_kernel(plan, *r),
        jax.ShapeDtypeStruct((rows, width, wide), F32),
        tuple(result),
        [pltpu.VMEM((rows, width, LANES), F32)] * 2,
        10**8,
    )
    return result[None]


def solution(mesh):
    placed = (
        P(None, "lat", None, "ch"),
        P(None, "ch"),
        P(None, "ch"),
        P(None, "ch", None, None),
        P(None, "ch", None),
        P(None, "ch", None, None),
        P(None, "ch", None),
        P(None, "ch"),
        P("ch"),
        P("ch", None),
    )

    return jax.shard_map(
        local, mesh=mesh, in_specs=placed, out_specs=P(None, "lat", None, "ch"), check_vma=False
    )
```

```python
import math

import jax
import jax.numpy as jnp
import numpy as np
from jax import lax
from jax.experimental import pallas as pl
from jax.experimental.pallas import tpu as pltpu
from jax.sharding import PartitionSpec as P


D = 768
M = 64
STEPS = 4
EPS = 1e-05
SHRINK = 0.01
HALF = 64
PACK, START, FIRST = 24, 24, 58
PART = 4
LANES = 128
BF = jnp.bfloat16
F32 = jnp.float32


class Plan:
    def __init__(self, lat, ch, rows, width):
        self.lat, self.ch, self.rows, self.width = lat, ch, rows, width
        self.height = rows * lat
        self.short = width // ch
        self.padded = -(-self.short // 16) * 16
        self.tokens = rows * self.padded
        self.classes = self.short // 2 + 1
        self.per = -(-self.classes // lat)
        self.wide = D // ch
        self.units = self.wide // HALF
        self.items = rows * self.per
        spare = self.items % 8
        if self.items > 8 and spare and spare * self.units <= 8:
            self.main, self.left = self.items - spare, spare
        else:
            self.main, self.left = -(-self.items // 8) * 8, 0
        self.message = self.units * self.main + (8 if self.left else 0)
        slots = 0
        while (slots // 2) * self.short + (slots % 2) * (self.short - self.short // 2) < M:
            slots += 1
        self.slots = slots
        self.modes = self.per * slots * self.height
        self.peers = lat * ch
        self.spare = self.padded - self.short
        self.packed = self.tokens + self.tokens // 2
        hj = np.arange(self.main)
        self.item_h = np.where(hj < self.items, hj // self.per, 0)
        self.item_j = np.where(hj < self.items, hj % self.per, -1)
        tail = self.main + np.arange(self.left)
        self.tail_h, self.tail_j = tail // self.per, tail % self.per


def split_np(table):
    hi = table.astype(np.float32).astype(BF)
    lo = (table - hi.astype(np.float64)).astype(np.float32).astype(BF)
    return hi, lo


def short_tables(plan):
    g = np.arange(plan.lat)
    item_g = np.concatenate([np.repeat(g, plan.main), np.repeat(g, plan.left)])
    item_h = np.concatenate([np.tile(plan.item_h, plan.lat), np.tile(plan.tail_h, plan.lat)])
    item_j = np.concatenate([np.tile(plan.item_j, plan.lat), np.tile(plan.tail_j, plan.lat)])
    order = item_g * plan.per + item_j
    good = (item_j >= 0) & (order < plan.classes)
    tok_h = np.repeat(np.arange(plan.rows), plan.padded)
    tok_a = np.tile(np.arange(plan.padded), plan.rows)
    mask = good[:, None] & (item_h[:, None] == tok_h[None]) & (tok_a[None] < plan.short)
    angle = 2 * np.pi / plan.short * (order[:, None] * tok_a[None] % plan.short)
    cos, sin = np.cos(angle) * mask, np.sin(angle) * mask
    forward = np.concatenate([cos, -sin], 0)
    inverse = np.concatenate([cos.T, -sin.T], 1)
    side = max(forward.shape)
    tables = [np.pad(t, [(0, side - n) for n in t.shape]) for t in (forward, inverse)]
    return np.stack(split_np(tables[0]) + split_np(tables[1]))


def mode_places(plan):
    j, t, k = (
        v.reshape(-1)
        for v in np.meshgrid(
            np.arange(plan.per), np.arange(plan.slots), np.arange(plan.height), indexing="ij"
        )
    )
    peer = np.arange(plan.peers)
    col_p = np.concatenate([np.repeat(peer, plan.main), np.repeat(peer, plan.left)])
    col_h = np.concatenate([np.tile(plan.item_h, plan.peers), np.tile(plan.tail_h, plan.peers)])
    col_j = np.concatenate([np.tile(plan.item_j, plan.peers), np.tile(plan.tail_j, plan.peers)])
    col_h = (col_p // plan.ch) * plan.rows + col_h
    none = np.zeros_like(j)
    row = np.stack([j, t % 2, (t + 1) // 2, k] + [none] * 4).astype(np.float32)
    none = np.zeros_like(col_p)
    col = np.stack([col_p % plan.ch, col_h, col_j] + [none] * 5).astype(np.float32)
    return row, col


def cos_sin(turns):
    turns = turns - jnp.floor(turns + 0.5)
    quarter = jnp.floor(turns * 4.0 + 0.5)
    x = (turns - quarter * 0.25) * (2.0 * math.pi)
    y = x * x
    sin = x * (1 + y * (-1 / 6 + y * (1 / 120 + y * (-1 / 5040 + y * (1 / 362880)))))
    cos = 1 + y * (-0.5 + y * (1 / 24 + y * (-1 / 720 + y * (1 / 40320 - y * (1 / 3628800)))))
    odd = jnp.abs(quarter) == 1.0
    c, s = jnp.where(odd, sin, cos), jnp.where(odd, cos, sin)
    c = jnp.where((quarter == 1.0) | (jnp.abs(quarter) == 2.0), -c, c)
    s = jnp.where((quarter == -1.0) | (jnp.abs(quarter) == 2.0), -s, s)
    return c, s


def mode_table(plan, first_class, row, col):
    j, odd, times, k = row
    q, h, col_j = col
    order = first_class + j
    mode = times * plan.short + jnp.where(odd == 1.0, -order, order)
    fine = (mode < M) & (order < plan.classes)
    fine = fine & ((order > 0.0) | (times == 0.0) | (odd == 1.0))
    fine = fine & ((2.0 * order != plan.short) | (odd == 0.0))
    scale = 1.0 / math.sqrt(plan.height * plan.width)
    weight = jnp.where(fine, scale, 0.0)
    doubled = jnp.where(mode == 0.0, 1.0, 2.0)
    turn = jnp.where(odd == 1.0, 1.0, -1.0)
    product = k * h
    product = product - plan.height * jnp.floor(product * (1.0 / plan.height) + 1e-4)
    cos, sin = cos_sin(mode * q * (1.0 / plan.width) + product * (1.0 / plan.height))
    keep = jnp.where(j == col_j, weight, 0.0)
    return cos * keep, sin * (keep * turn), doubled


def split(value):
    hi = value.astype(BF)
    return hi, (value - hi.astype(F32)).astype(BF)


def dot(a, b):
    return jnp.dot(a, b, preferred_element_type=F32)


def low_lanes(shape):
    return lax.broadcasted_iota(jnp.int32, shape, len(shape) - 1) % LANES < HALF


def swap(value):
    return pltpu.roll(value, HALF, 1)


def norm(values, gain, shift):
    mean = jnp.sum(values, -1, keepdims=True) * (1.0 / D)
    spread = jnp.sum(values * values, -1, keepdims=True) * (1.0 / D) - mean * mean
    return (values - mean) * lax.rsqrt(spread + EPS) * gain + shift


def emit_wire(plan, normed, tab, wire_ref, scratch):
    hi, lo = split(normed)
    count = plan.lat * plan.main
    half = count + plan.lat * plan.left
    fhi, flo = tab[0, : 2 * half, : plan.tokens], tab[1, : 2 * half, : plan.tokens]
    spec = dot(fhi, hi) + dot(flo, hi) + dot(fhi, lo)
    low = low_lanes((half, LANES))
    for tile in range(D // LANES):
        lanes = slice(tile * LANES, (tile + 1) * LANES)
        re, im = spec[:half, lanes], spec[half:, lanes]
        pair = (jnp.where(low, re, swap(im)), jnp.where(low, swap(re), im))
        for which in range(2):
            c, u = divmod(2 * tile + which, plan.units)
            part = pair[which]
            scratch[:, c, u * plan.main : (u + 1) * plan.main, :] = part[:count].reshape(
                plan.lat, plan.main, LANES
            )
            for spot in range(plan.left):
                row = plan.units * plan.main + u * plan.left + spot
                for g in range(plan.lat):
                    at = count + g * plan.left + spot
                    scratch[g, c, row : row + 1, :] = part[at : at + 1]
    if plan.left:
        first = plan.units * (plan.main + plan.left)
        if first < plan.message:
            scratch[:, :, first:, :] = jnp.zeros(
                (plan.lat, plan.ch, plan.message - first, LANES), F32
            )
    wire_ref[...] = scratch[...].reshape(plan.peers, plan.message, LANES).astype(BF)


def read_wire(plan, wire_ref, tab, scratch):
    scratch[...] = wire_ref[...].astype(F32).reshape(plan.lat, plan.ch, plan.message, LANES)
    count = plan.lat * plan.main
    half = count + plan.lat * plan.left
    low = low_lanes((half, LANES))

    def unit(index):
        c, u = divmod(index, plan.units)
        parts = [scratch[:, c, u * plan.main : (u + 1) * plan.main, :].reshape(count, LANES)]
        for g in range(plan.lat):
            for spot in range(plan.left):
                row = plan.units * plan.main + u * plan.left + spot
                parts.append(scratch[g, c, row : row + 1, :])
        return jnp.concatenate(parts, 0) if len(parts) > 1 else parts[0]

    tiles = []
    for tile in range(D // LANES):
        a, b = unit(2 * tile), unit(2 * tile + 1)
        re = jnp.where(low, a, swap(b))
        im = jnp.where(low, swap(a), b)
        tiles.append(jnp.concatenate([re, im], 0).astype(BF))
    right = jnp.concatenate(tiles, 1)
    ghi, glo = tab[2, : plan.tokens, : 2 * half], tab[3, : plan.tokens, : 2 * half]
    return dot(ghi, right) + dot(glo, right)


def pack(values):
    half = values.shape[0] // 2
    tail = values[:, LANES:]
    return jnp.concatenate([values[:, :LANES], jnp.concatenate([tail[:half], tail[half:]], 1)], 0)


def unpack(message):
    tokens = message.shape[0] // 3 * 2
    tail = message[tokens:]
    tail = jnp.concatenate([tail[:, :HALF], tail[:, HALF:]], 0)
    return jnp.concatenate([message[:tokens], tail], 1)


def pack_kernel(plan, state_ref, gain_hbm, bias_hbm, up_hbm, *refs):
    outs, (scratch, body, tail, out_ref, gain_ref, bias_ref, up_ref, sem) = refs[: plan.ch], refs[plan.ch :]
    copies = fetch([gain_hbm, bias_hbm, up_hbm], [gain_ref, bias_ref, up_ref], sem)
    body[...] = state_ref[:, :, :LANES]
    tail[:, :, :HALF] = state_ref[:, :, LANES:]
    for copy in copies:
        copy.wait()
    line = up_ref[...].astype(F32).reshape(1, -1)
    small = [gain_ref[...].astype(F32), bias_ref[...].astype(F32)]
    small += [line[:, n * plan.wide : (n + 1) * plan.wide] for n in range(plan.ch)]
    small = jnp.concatenate(small, 0)
    count = small.shape[0]
    scratch[...] = jnp.zeros(scratch.shape, F32)
    for n in range(count):
        h, s = divmod(n, plan.spare)
        at = h * plan.padded + plan.short + s
        scratch[at : at + 1, :] = small[n : n + 1]
    for q in range(plan.ch):
        for h in range(plan.rows):
            at = h * plan.padded
            every = pl.ds(q, plan.short, stride=plan.ch)
            scratch[at : at + plan.short, :LANES] = body[h, every, :]
            scratch[at : at + plan.short, LANES:] = tail[h, every, :][:, :HALF]
        out_ref[q] = pack(scratch[...])
    for n in range(plan.ch):
        outs[n][...] = out_ref[lax.axis_index("ch") ^ n]


def unpack_kernel(plan, *refs):
    got, (out_ref, body, tail) = refs[: plan.ch], refs[plan.ch :]
    for n in range(plan.ch):
        q = lax.axis_index("ch") ^ n
        values = unpack(got[n][...])
        wide = jnp.concatenate([values[:, LANES:], values[:, LANES:]], 1)
        for h in range(plan.rows):
            at = slice(h * plan.padded, h * plan.padded + plan.short)
            every = pl.ds(q, plan.short, stride=plan.ch)
            body[h, every, :] = values[at, :LANES]
            tail[h, every, :] = wide[at]
    out_ref[:, :, :LANES] = body[...]
    out_ref[:, :, LANES:] = tail[:, :, :HALF]


def fetch(sources, targets, sem):
    copies = [pltpu.make_async_copy(a, b, sem.at[n]) for n, (a, b) in enumerate(zip(sources, targets))]
    for copy in copies:
        copy.start()
    return copies


def parts_kernel(up_ref, down_ref, up_out, own_out, rest_out, *refs):
    mids, sem = refs[:3], refs[3]
    half, own = up_out.shape[1], own_out.shape[0]
    side = lax.axis_index("lat") % 2
    at = pl.multiple_of(side * half, LANES)
    to = pl.multiple_of(side * own, HALF)
    into = fetch(
        [up_ref.at[:, pl.ds(at, half)], down_ref.at[pl.ds(to, own), :], down_ref.at[2 * own :, :]],
        mids,
        sem,
    )
    away = []
    for n, out in enumerate((up_out, own_out, rest_out)):
        into[n].wait()
        away.append(pltpu.make_async_copy(mids[n], out, sem.at[3 + n]))
        away[n].start()
    for copy in away:
        copy.wait()


def fill_tables(plan, rowv, colv, rowt, colt, chi, clo, ehi, elo):
    first = (lax.axis_index("lat") * plan.per).astype(F32)
    size = plan.modes
    wide = plan.peers * (plan.main + plan.left)
    rows = [rowv[:, n : n + 1] for n in range(4)]
    cols = [colv[n : n + 1, :] for n in range(3)]
    cos, sin, _ = mode_table(plan, first, rows, cols)
    chi[:, :wide], clo[:, :wide] = split(cos)
    chi[:, wide:], clo[:, wide:] = split(sin)
    rows = [rowt[n : n + 1, :] for n in range(4)]
    cols = [colt[:, n : n + 1] for n in range(3)]
    cos, sin, doubled = mode_table(plan, first, rows, cols)
    ehi[:, :size], elo[:, :size] = split(cos * doubled)
    ehi[:, size:], elo[:, size:] = split(-sin * doubled)


def high_units(plan):
    return plan.units - 1


def block_kernel(plan, fin, finb, fout, foutb, *refs):
    outs, (w1h, w1l, w2h, w2l, b1, b2), sem = refs[:6], refs[6:12], refs[12]
    copies = [pltpu.make_async_copy(a, b, sem.at[n]) for n, (a, b) in enumerate(zip(refs[6:12], outs))]
    span = high_units(plan)
    for weights, bias, high, low, out in ((fin, finb, w1h, w1l, b1), (fout, foutb, w2h, w2l, b2)):
        blocks, channels = weights.shape[1], weights.shape[2]
        for n in range(blocks):
            full = []
            for p in range(2):
                lines = [jnp.zeros((channels, blocks * channels), F32)] * blocks
                cells = [jnp.zeros((channels, channels), F32)] * blocks
                cells[n] = weights[p, n]
                lines[n] = jnp.concatenate(cells, 1)
                full.append(jnp.concatenate(lines, 0))
            for u in range(n, n + span):
                at = slice(u * HALF, (u + 1) * HALF)
                real, imag = full[0][at], full[1][at]
                for p, (left, right) in enumerate(((real, imag), (-imag, real))):
                    cells = []
                    for v in range(n, n + span):
                        cut = slice(v * HALF, (v + 1) * HALF)
                        cells += [left[:, cut], right[:, cut]]
                    row = jnp.concatenate(cells, 1)
                    to = slice((2 * (u - n) + p) * HALF, (2 * (u - n) + p + 1) * HALF)
                    high[n, to, :], low[n, to, :] = split(row)
        lines = [jnp.concatenate([bias[p, n : n + 1] for n in range(blocks)], 1) for p in range(2)]
        cells = []
        for v in range(plan.units):
            cells += [line[:, v * HALF : (v + 1) * HALF] for line in lines]
        out[...] = jnp.concatenate(cells, 1)
    for copy in copies:
        copy.start()
    for copy in copies:
        copy.wait()


def start_kernel(plan, *refs):
    came, (tab_hbm, begun_hbm, wire_ref, scratch, got_ref, tab, begun, sem) = refs[: plan.ch], refs[plan.ch :]
    for n in range(plan.ch):
        got_ref[lax.axis_index("ch") ^ n] = came[n][...]
    sum_ref, par_ref = begun.at[: plan.tokens], begun.at[plan.tokens : plan.tokens + 16]
    bias_ref = par_ref.at[8:16]
    copies = fetch([tab_hbm], [tab], sem)
    got = [unpack(got_ref[c]) for c in range(plan.ch)]
    full = jnp.concatenate(got, 1)
    rows = []
    for h in range(plan.rows):
        for s in range(plan.spare):
            rows.append(h * plan.padded + plan.short + s)
    for n in range(5):
        par_ref[n : n + 1, :] = full[rows[n] : rows[n] + 1, :]
    par_ref[5:8, :] = jnp.zeros((3, D), F32)
    bias_ref[...] = jnp.zeros(bias_ref.shape, F32)
    for s in range(plan.ch):
        source = unpack(came[s][...])
        parts = [source[rows[5 + n] : rows[5 + n] + 1, :] for n in range(plan.ch)]
        line = jnp.concatenate(parts, 1)
        bias_ref[s : s + 1, :] = line
    inside = lax.broadcasted_iota(jnp.int32, (plan.tokens, 1), 0) % plan.padded < plan.short
    values = jnp.where(inside, full, 0.0)
    normed = norm(values, par_ref[0:1, :], par_ref[2:3, :])
    sum_ref[...] = values + normed
    copies[0].wait()
    side = tab.shape[1]
    rows = slice(plan.tokens + 16, plan.tokens + 16 + side)
    for n in range(2):
        whole = tab[2 * n].astype(F32) + tab[2 * n + 1].astype(F32)
        begun[rows, 256 * n : 256 * n + side] = whole
    copies.append(pltpu.make_async_copy(begun, begun_hbm, sem.at[1]))
    copies[1].start()
    emit_wire(plan, normed, tab, wire_ref, scratch)
    copies[1].wait()


def token_kernel(plan, first, last, *refs):
    copies = []
    if first:
        wire_in, sources, refs = refs[0], refs[1:16], refs[16:]
        (sum_out, wire_out, par_out, up_all, down_all), refs = refs[:5], refs[5:]
        scratch, sem, (begun, tab) = refs[0], refs[1], refs[2:]
        sum_in, par_ref = begun.at[: plan.tokens], begun.at[plan.tokens : plan.tokens + 16]
        shard = up_all.shape[1] // plan.ch
        half, own = shard // 2, shard // PART
        y = lax.axis_index("lat") % 2
        copies = fetch(sources[:1], (begun,), sem)
        groups = []
        weights = sources[1:]
        for s in range(plan.ch):
            at = s * shard
            if s < plan.ch // 2:
                ups, downs = weights[:1], weights[1:2]
                weights = weights[2:]
                ups = [(ups[0], up_all.at[:, at : at + shard])]
                downs = [(downs[0], down_all.at[at : at + shard, :])]
            else:
                ups, downs = weights[:2], weights[2:5]
                spots = [pl.multiple_of(at + n * half, LANES) for n in (y, 1 - y)]
                ups = [(w, up_all.at[:, pl.ds(n, half)]) for w, n in zip(ups, spots)]
                spots = [pl.multiple_of(at + n * own, HALF) for n in (y, 1 - y)]
                spots.append(at + 2 * own)
                sizes = (own, own, shard - 2 * own)
                downs = [
                    (w, down_all.at[pl.ds(n, size), :]) for w, n, size in zip(downs, spots, sizes)
                ]
                weights = weights[5:]
            group = []
            for source, target in ups + downs:
                count = len(copies)
                copies.append(pltpu.make_async_copy(source, target, sem.at[count]))
                copies[-1].start()
                group.append(copies[-1])
            groups.append(group)
        copies[0].wait()
        side = tab.shape[1]
        for n in range(2):
            whole = begun[plan.tokens + 16 :, 256 * n : 256 * n + side]
            tab[2 * n], tab[2 * n + 1] = split(whole)
        par_out[...] = par_ref[...]
    else:
        wire_in, sum_in, tab, par_ref, up_all, down_all = refs[:6]
        outs, scratch = refs[6:], refs[-1]
        if last:
            outs, scratch = refs[6:], refs[-2]
        shard = up_all.shape[1] // plan.ch
        half = shard // 2
    values = sum_in[...] + read_wire(plan, wire_in, tab, scratch)
    normed = norm(values, par_ref[1:2, :], par_ref[3:4, :]).astype(BF)
    mixed = par_ref[4:5, :]
    for s in range(2 * plan.ch):
        if first and s % 2 == 0:
            for copy in groups[s // 2]:
                copy.wait()
        at = slice((s % 2) * half, (s % 2 + 1) * half)
        cut = slice(s * half, (s + 1) * half)
        bias = par_ref[8 + s // 2 : 9 + s // 2, at]
        pre = dot(normed, up_all[:, cut]) + bias
        hidden = (0.5 * pre * (1.0 + lax.erf(pre * math.sqrt(0.5)))).astype(BF)
        mixed = mixed + dot(hidden, down_all[cut, :])
    values = values + mixed
    if last:
        for c in range(plan.ch):
            refs[-1][c] = pack(values[:, c * plan.wide : (c + 1) * plan.wide])
        for n in range(plan.ch):
            outs[n][...] = refs[-1][lax.axis_index("ch") ^ n]
        return
    if not first:
        sum_out, wire_out = outs[:2]
    normed = norm(values, par_ref[0:1, :], par_ref[2:3, :])
    sum_out[...] = values + normed
    emit_wire(plan, normed, tab, wire_out, scratch)


def spectral_kernel(plan, far, wire_in, *refs):
    copies, away = [], []
    if far:
        places, sign_ref, sources, wire_out = refs[:4], refs[4], refs[5:11], refs[11]
        outs, scratch, sem = refs[12:16], refs[16], refs[17]
        chi, clo, ehi, elo = tables = refs[18:22]
        w1h, w1l, w2h, w2l, b1, b2 = mids = refs[22:]
        copies = fetch(sources, mids, sem)
        fill_tables(plan, *places, *tables)
        for n, (table, out) in enumerate(zip(tables, outs)):
            away.append(pltpu.make_async_copy(table, out, sem.at[6 + n]))
            away[n].start()
    else:
        chi, clo, ehi, elo, w1h, w1l, w2h, w2l, b1, b2, sign_ref, wire_out, scratch = refs
    scratch[...] = wire_in[...].astype(F32)
    count = plan.peers * plan.main
    half = count + plan.peers * plan.left
    low = low_lanes((half, LANES))
    pieces = []
    for u in range(plan.units):
        parts = [scratch[:, u * plan.main : (u + 1) * plan.main, :].reshape(count, LANES)]
        for p in range(plan.peers if plan.left else 0):
            row = plan.units * plan.main + u * plan.left
            parts.append(scratch[p, row : row + plan.left, :])
        data = jnp.concatenate(parts, 0) if len(parts) > 1 else parts[0]
        turned = swap(data)
        turned = jnp.where(low, -turned, turned)
        pieces.append(jnp.concatenate([data, turned], 0).astype(BF))
    right = jnp.concatenate(pieces, 1)

    def ready(*which):
        for n in which if far else ():
            copies[n].wait()

    spec = dot(chi[...], right) + dot(clo[...], right)
    sign = jnp.concatenate([sign_ref[...]] * plan.units, 1)
    spec = spec * sign

    def layer(value, wh, wl, bias):
        hi, lo = split(value)
        span, total = wh.shape[1], 0.0
        for n in range(wh.shape[0]):
            cut = slice(n * LANES, n * LANES + span)
            part = dot(hi[:, cut], wh[n]) + dot(hi[:, cut], wl[n]) + dot(lo[:, cut], wh[n])
            sides = [(part.shape[0], n * LANES), (part.shape[0], value.shape[1] - span - n * LANES)]
            cells = [jnp.zeros(sides[0], F32)] * (n > 0) + [part]
            cells += [jnp.zeros(sides[1], F32)] * (sides[1][1] > 0)
            total = total + jnp.concatenate(cells, 1)
        return total + bias[...]

    ready(0, 1, 4)
    first = jnp.maximum(layer(spec, w1h, w1l, b1), 0.0)
    ready(2, 3, 5)
    second = layer(first, w2h, w2l, b2)
    shrunk = jnp.where(
        second > SHRINK, second - SHRINK, jnp.where(second < -SHRINK, second + SHRINK, 0.0)
    )
    shrunk = shrunk * sign
    low = low_lanes((plan.modes, LANES))
    pieces = []
    for u in range(plan.units):
        part = shrunk[:, u * LANES : (u + 1) * LANES]
        turned = swap(part)
        pieces.append(jnp.concatenate([part, jnp.where(low, -turned, turned)], 0))
    hi, lo = split(jnp.concatenate(pieces, 1))
    back = dot(ehi[...], hi) + dot(elo[...], hi) + dot(ehi[...], lo)
    for u in range(plan.units):
        part = back[:, u * LANES : (u + 1) * LANES]
        scratch[:, u * plan.main : (u + 1) * plan.main, :] = part[:count].reshape(
            plan.peers, plan.main, LANES
        )
        row = plan.units * plan.main + u * plan.left
        for p in range(plan.peers if plan.left else 0):
            at = count + p * plan.left
            scratch[p, row : row + plan.left, :] = part[at : at + plan.left]
    wire_out[...] = scratch[...].astype(BF)
    for copy in away:
        copy.wait()


def call(body, outs, operands, scratch, flops, far_in=0, far_out=(), grant=20):
    vmem = pl.BlockSpec(memory_space=pltpu.VMEM)
    anywhere = pl.BlockSpec(memory_space=pl.ANY)
    flat, tree = jax.tree.flatten(outs)
    out_specs = [anywhere if n in far_out else vmem for n in range(len(flat))]
    return pl.pallas_call(
        body,
        out_shape=outs,
        in_specs=[vmem] * (len(operands) - far_in) + [anywhere] * far_in,
        out_specs=jax.tree.unflatten(tree, out_specs),
        scratch_shapes=scratch,
        compiler_params=pltpu.CompilerParams(vmem_limit_bytes=grant * 2**20),
        cost_estimate=pl.CostEstimate(flops=flops, bytes_accessed=2**20, transcendentals=0),
    )(*operands)


def local(
    state,
    norm_gains,
    channel_biases,
    filter_in,
    filter_in_bias,
    filter_out,
    filter_out_bias,
    up_weight,
    up_bias,
    down_weight,
):
    _, rows, width, wide = state.shape
    plan = Plan(lax.axis_size("lat"), lax.axis_size("ch"), rows, width)
    ch = plan.ch
    far = ch // 2
    both = ("lat", "ch")
    assert plan.spare * rows >= 5 + ch and up_bias.shape[0] == ch * wide

    def across(value, step):
        return lax.ppermute(value, "ch", [(i, i ^ step) for i in range(ch)])

    def beside(value):
        return lax.ppermute(value, "lat", [(i, i ^ 1) for i in range(plan.lat)])

    def exchange(value, axes):
        return lax.all_to_all(value, axes, 0, 0, tiled=True)

    def after(value, token):
        return lax.optimization_barrier((value, token))[0]

    message = (jax.ShapeDtypeStruct((plan.packed, LANES), F32),) * ch
    mail = pltpu.VMEM((ch, plan.packed, LANES), F32)
    tokens = call(
        lambda *r: pack_kernel(plan, *r),
        message,
        (state[0], norm_gains, channel_biases, up_bias),
        [pltpu.VMEM((plan.tokens, wide), F32)]
        + [pltpu.VMEM((rows, width, LANES), F32)] * 2
        + [mail]
        + [pltpu.VMEM(v.shape, BF) for v in (norm_gains, channel_biases, up_bias)]
        + [pltpu.SemaphoreType.DMA((3,))],
        10**8,
        far_in=3,
        grant=PACK,
    )
    got = [tokens[0]] + [across(tokens[n], n) for n in range(1, ch)]

    half, own = up_weight.shape[1] // 2, down_weight.shape[0] // PART
    shapes = [(D, half), (own, D), (down_weight.shape[0] - 2 * own, D)]
    parts = [jax.ShapeDtypeStruct(shape, BF) for shape in shapes]
    up_part, own_part, rest_part = call(
        parts_kernel,
        tuple(parts),
        (up_weight, down_weight),
        [pltpu.VMEM(t.shape, BF) for t in parts] + [pltpu.SemaphoreType.DMA((6,))],
        10**6,
        far_in=2,
        far_out=(0, 1, 2),
        grant=58,
    )
    up_a = across(up_part, far)
    span = LANES * high_units(plan)
    blocks = [jax.ShapeDtypeStruct((filter_in.shape[1], span, span), BF)] * 4
    blocks += [jax.ShapeDtypeStruct((1, 2 * wide), F32)] * 2
    blocks = call(
        lambda *r: block_kernel(plan, *r),
        tuple(blocks),
        (filter_in, filter_in_bias, filter_out, filter_out_bias),
        [pltpu.VMEM(t.shape, t.dtype) for t in blocks] + [pltpu.SemaphoreType.DMA((6,))],
        10**8,
        far_out=range(6),
        grant=58,
    )
    got[1], *blocks = lax.optimization_barrier((got[1], *blocks))
    up_c, down_c = across(up_weight, 1), across(down_weight, 1)

    short = jnp.asarray(short_tables(plan))
    odd = np.tile(np.repeat(np.arange(plan.slots) % 2, plan.height), plan.per)
    sign = np.where((odd[:, None] == 1) & (np.arange(LANES)[None] >= HALF), -1.0, 1.0)
    sign = sign.astype(np.float32)

    wire = jax.ShapeDtypeStruct((plan.peers, plan.message, LANES), BF)
    held = jax.ShapeDtypeStruct((plan.tokens, D), F32)
    scratch = [pltpu.VMEM((plan.lat, ch, plan.message, LANES), F32)]
    begun = jax.ShapeDtypeStruct((plan.tokens + 16 + short.shape[1], D), F32)
    assert short.shape[1] <= D - 256
    begun, sent = call(
        lambda *r: start_kernel(plan, *r),
        (begun, wire),
        (*got, short),
        scratch
        + [mail]
        + [pltpu.VMEM(t.shape, t.dtype) for t in (short, begun)]
        + [pltpu.SemaphoreType.DMA((2,))],
        10**9,
        far_in=1,
        far_out=(0,),
        grant=START,
    )
    row, col = mode_places(plan)
    lines = plan.peers * (plan.main + plan.left)
    dims = [(plan.modes, 2 * lines)] * 2 + [(lines, 2 * plan.modes)] * 2
    tables = [jax.ShapeDtypeStruct(shape, BF) for shape in dims]
    for step_index in range(STEPS):
        first, last = step_index == 0, step_index == STEPS - 1
        arrived = exchange(sent, both)
        if first:
            down_a = across(own_part, far)
            rest = across(rest_part, far)
            up_b = beside(up_a)
            up_ac = across(up_a, 1)
        if first:
            sent, *tables = call(
                lambda *r: spectral_kernel(plan, True, *r),
                (wire, *tables),
                (arrived, row.T, col, row, col.T, sign, *blocks),
                [pltpu.VMEM((plan.peers, plan.message, LANES), F32)]
                + [pltpu.SemaphoreType.DMA((10,))]
                + [pltpu.VMEM(t.shape, t.dtype) for t in (*tables, *blocks)],
                10**9,
                far_in=6,
                far_out=range(1, 5),
                grant=FIRST,
            )
        else:
            sent = call(
                lambda *r: spectral_kernel(plan, False, *r),
                wire,
                (arrived, *tables, *blocks, sign),
                [pltpu.VMEM((plan.peers, plan.message, LANES), F32)],
                10**9,
            )
        if first:
            up_bc = across(after(up_b, sent), 1)
            down_b = beside(after(down_a, sent))
            down_ac = across(after(down_a, sent), 1)
            down_bc = across(after(down_b, sent), 1)
            rest_c = across(after(rest, sent), 1)
        arrived = exchange(sent, both)
        if first:
            near = (up_weight, down_weight, up_c, down_c)
            distant = (up_a, up_b, down_a, down_b, rest, up_ac, up_bc, down_ac, down_bc, rest_c)
            sources = (begun, *near, *distant)
            total, sent, params, ups, downs = call(
                lambda *r: token_kernel(plan, True, False, *r),
                (
                    held,
                    wire,
                    jax.ShapeDtypeStruct((16, D), F32),
                    jax.ShapeDtypeStruct((D, ch * up_weight.shape[1]), BF),
                    jax.ShapeDtypeStruct((ch * down_weight.shape[0], D), BF),
                ),
                (arrived, *sources),
                scratch
                + [pltpu.SemaphoreType.DMA((len(sources),))]
                + [pltpu.VMEM(t.shape, t.dtype) for t in (begun, short)],
                10**10,
                        far_in=len(sources),
                grant=24,
            )
            continue
        result = call(
            lambda *r: token_kernel(plan, False, last, *r),
            message if last else (held, wire),
            (arrived, total, short, params, ups, downs),
            scratch + [mail] * last,
            10**10,
        )
        if not last:
            total, sent = result
    result = [result[0]] + [across(result[n], n) for n in range(1, ch)]
    result = call(
        lambda *r: unpack_kernel(plan, *r),
        jax.ShapeDtypeStruct((rows, width, wide), F32),
        tuple(result),
        [pltpu.VMEM((rows, width, LANES), F32)] * 2,
        10**8,
    )
    return result[None]


def solution(mesh):
    placed = (
        P(None, "lat", None, "ch"),
        P(None, "ch"),
        P(None, "ch"),
        P(None, "ch", None, None),
        P(None, "ch", None),
        P(None, "ch", None, None),
        P(None, "ch", None),
        P(None, "ch"),
        P("ch"),
        P("ch", None),
    )

    return jax.shard_map(
        local, mesh=mesh, in_specs=placed, out_specs=P(None, "lat", None, "ch"), check_vma=False
    )
```
